128 devices in a mesh: blk: 16 (over x, z), order: 8 (over y, core).
Axes of the slice: x: 4, y: 4, z: 4, core: 2. Of those that a mesh axis runs over, the one named last changes fastest.
Arguments:
- field: float32 [16, 1024, 4096], P(None, 'blk', 'order'), may hold values from -6 to 6
- ocean_mask: int32 [1024, 4096], P('blk', 'order'), may hold values from 0 to 1, as said below
- plan: int32 [1024], replicated, may hold values from 0 to 768, as said below
- legendre: bfloat16 [768, 1024, 1024], P('blk', 'order'), may hold values from -0.3125 to 0.3125
Outputs:
- coefficients: float32 [1024, 16, 2, 1024], P('blk', None, None, 'order')
The draws below stay inside these ranges and needn't reach their ends.
Inputs may be any that keep to these rules, and one draw needn't show every extreme that they name: `ocean_mask`: exactly 256 cycles are all land, at the ends of the cycle order; every other cycle has an ocean point. plan is 768 exactly at the cycles that are all land, and names every slot below 768 once at the other cycles; slot p belongs to index p // 48 of blk; the cycles of one index of blk name at most 4 slots of one index, and in every draw some index of blk names exactly 4 slots of some index.
All inputs are finite; a program needn't handle non-finite values.
Results may differ from the reference program's by a relative error of at most 0.0029.
Values may be sent and summed in bfloat16 or wider, within the bound.
A program may use at most 128 MiB of HBM per device.

```python
import jax
import jax.numpy as jnp
from jax import lax

NLON = 4096
M = 1024
L = 1024
FIELDS = 16
CYCLES = 1024
SLOT_DEV = 48
SLOTS = 768
N_BLK = 16
N_ORDER = 8


def wet_cycles(key):
    folded = jax.random.fold_in(key, 11)
    dry_count = CYCLES - SLOTS
    south = jax.random.randint(folded, (), 0, dry_count + 1)
    cycles = jnp.arange(CYCLES, dtype=jnp.int32)
    inside = (cycles >= south) & (cycles < CYCLES - dry_count + south)
    return inside.astype(jnp.int32)


def draw_plan(key, part):
    wet = wet_cycles(key)
    counted = jnp.cumsum(wet).astype(jnp.int32) - 1
    owner_slot = counted % N_BLK * SLOT_DEV + counted // N_BLK
    return jnp.where(wet == 1, owner_slot, SLOTS).astype(jnp.int32)


def draw_ocean_mask(key, part):
    wet = wet_cycles(key)
    levels = jax.random.randint(jax.random.fold_in(key, 12), (CYCLES, NLON), 0, 10)
    cycles = jnp.arange(CYCLES, dtype=jnp.int32)[:, None]
    longitudes = jnp.arange(NLON, dtype=jnp.int32)[None, :]
    forced = longitudes == cycles * 37 % NLON
    ocean = ((levels < 7) | forced) & (wet[:, None] == 1)
    return ocean.astype(jnp.int32)


def strengthened(drawn, own_key, source, target, shards_of, factor):
    owner, partner = [(jnp.arange(drawn.shape[dim]) // (drawn.shape[dim] // shards_of)).reshape([-1 if axis == dim else 1 for axis in range(drawn.ndim)]) for dim in (source, target)]
    chosen = jax.random.permutation(own_key, shards_of)[partner]
    strong = (owner == chosen) | (owner == (partner + shards_of // 2) % shards_of)
    return jnp.where(strong, factor * drawn, drawn)


def block_scale(stream_key, shape, cuts, least, high):
    gain = 1.0
    for position, blocks in cuts:
        steps = jax.random.uniform(jax.random.fold_in(jax.random.fold_in(stream_key, 6), position), (blocks,), jnp.float32, least / len(cuts), high / len(cuts))
        gain = gain * jnp.repeat(jnp.exp(steps), shape[position] // blocks).reshape((-1,) + (1,) * (len(shape) - 1 - position))
    return gain


def noise(key, shape, deviation, bound, shards=(), kind=jnp.bfloat16):
    result = deviation * jax.random.normal(key, shape, jnp.float32)
    if shards:
        result = result * block_scale(key, shape, shards, -0.22, 0.18)
    return jnp.clip(result, -bound, bound).astype(kind)


def gaussian_with(own_key, shape, scale, bound, shards, heavy, kind=jnp.bfloat16):
    drawn = scale * jax.random.normal(own_key, shape, jnp.float32)
    if shards:
        drawn = drawn * block_scale(own_key, shape, shards, -0.22, 0.18)
    return jnp.clip(strengthened(drawn, jax.random.fold_in(own_key, 3), *heavy), -bound, bound).astype(kind)


def setup_inputs(seed: int = 0) -> dict:
    key_list = jax.random.split(jax.random.key(seed), 5)
    field = noise(key_list[0], (FIELDS, CYCLES, NLON), 1.0, 6.0, ((1, 16), (2, 8)), jnp.float32)
    ocean_mask = draw_ocean_mask(jax.random.fold_in(key_list[4], 71), 0)
    plan = draw_plan(jax.random.fold_in(key_list[4], 71), 0)
    legendre = gaussian_with(key_list[3], (SLOTS, M, L), SLOTS ** -0.5, 0.3125, ((0, 16), (1, 8)), (0, 2, 16, 2.0))
    return dict(field=field, ocean_mask=ocean_mask, plan=plan, legendre=legendre)


def reference(field, ocean_mask, plan, legendre):
    masked = field * ocean_mask.astype(jnp.float32)[None]
    holder = jnp.zeros((FIELDS, SLOTS + 1, NLON), jnp.float32)
    packed = holder.at[:, plan.astype(jnp.int32), :].set(masked)[:, :SLOTS]
    transform = jnp.fft.rfft(packed, axis=2)[:, :, :M] / jnp.sqrt(jnp.float32(NLON))
    spectrum = jnp.stack([jnp.real(transform), jnp.imag(transform)], axis=2).astype(jnp.float32).astype(jnp.bfloat16)
    width = M // N_ORDER

    def one_block(block_index):
        first = (block_index * width).astype(jnp.int32)
        table = lax.dynamic_slice_in_dim(legendre, first, width, 1).astype(jnp.float32)
        values = lax.dynamic_slice_in_dim(spectrum, first, width, 3).astype(jnp.float32)
        return jnp.einsum('pml,fpcm->lfcm', table, values)
    blocks = lax.map(one_block, jnp.arange(N_ORDER, dtype=jnp.int32))
    moved = jnp.moveaxis(blocks, 0, 3)
    return moved.reshape(L, FIELDS, 2, M)
```

```python
import math

import jax
import jax.numpy as jnp
from jax import lax
from jax.experimental import pallas as pl
from jax.experimental.pallas import tpu as pltpu
from jax.sharding import PartitionSpec as P

NLON = 4096
M = 1024


def twiddle(first, count):
    longitudes = first + jnp.arange(count, dtype=jnp.int32)
    orders = jnp.arange(M, dtype=jnp.int32)
    product = longitudes[:, None] * orders[None, :] % NLON
    angle = product.astype(jnp.float32) * (2.0 * math.pi / NLON)
    scale = 1.0 / math.sqrt(NLON)
    return jnp.stack([jnp.cos(angle) * scale, -jnp.sin(angle) * scale], axis=1)


def transform(values, table):
    return jnp.einsum("frn,ncm->frcm", values, table, precision=lax.Precision.HIGHEST)


def pack_cycles(masked, plan, slot_dev):
    n_blk = lax.axis_size("blk")
    own_index = lax.axis_index("blk")
    cycle_dev = masked.shape[1]
    cap = (cycle_dev + n_blk - 1) // n_blk
    grid = plan.reshape(n_blk, cycle_dev)
    owner = grid // slot_dev
    positions = jnp.arange(cycle_dev, dtype=jnp.int32)
    earlier = positions[None, :] < positions[:, None]
    same_owner = owner[:, :, None] == owner[:, None, :]
    rank = jnp.sum(same_owner & earlier[None], axis=2, dtype=jnp.int32)
    send_pos = owner * cap + rank
    local_pos = lax.dynamic_index_in_dim(send_pos, own_index, 0, keepdims=False)
    buffer_ids = jnp.arange(n_blk * cap, dtype=jnp.int32)
    send_onehot = (buffer_ids[:, None] == local_pos[None, :]).astype(jnp.float32)
    outgoing = jnp.einsum("qr,frn->fqn", send_onehot, masked, precision=lax.Precision.HIGHEST)
    arrived = lax.all_to_all(outgoing, "blk", split_axis=1, concat_axis=1, tiled=True)
    source_pos = (jnp.arange(n_blk, dtype=jnp.int32)[:, None] * cap + rank).reshape(-1)
    mine = (owner == own_index).reshape(-1)
    slot_local = (grid % slot_dev).reshape(-1)
    slot_ids = jnp.arange(slot_dev, dtype=jnp.int32)
    slot_onehot = ((slot_local[None, :] == slot_ids[:, None]) & mine[None, :]).astype(jnp.float32)
    source_onehot = (source_pos[:, None] == buffer_ids[None, :]).astype(jnp.float32)
    receive_map = jnp.dot(slot_onehot, source_onehot, precision=lax.Precision.HIGHEST)
    return jnp.einsum("pq,fqn->fpn", receive_map, arrived, precision=lax.Precision.HIGHEST)


MESH = pl.DeviceIdType.MESH
BF = jnp.bfloat16
F32 = jnp.float32
NBLOCK = 8


def contract_kernel(spec_ref, e_ref, leg_hbm, out_ref, leg, q, q2, ms1, mr1, ss1, sr1, ms2, mr2, ss2, sr2,
                    leg_sem, s_sem, r_sem):
    me = lax.axis_index("blk")
    x = me // 4
    z = me % 4
    for t in range(8):
        pltpu.make_async_copy(leg_hbm.at[:, pl.ds(16 * t, 16), :], leg.at[t], leg_sem.at[t]).start()
    barrier = pltpu.get_barrier_semaphore()
    for nx, nz in ((1, 0), (3, 0), (0, 1), (0, 3)):
        pl.semaphore_signal(barrier, inc=1, device_id={"blk": (x + nx) % 4 * 4 + (z + nz) % 4}, device_id_type=MESH)
    pl.semaphore_wait(barrier, 4)

    rows = lax.broadcasted_iota(jnp.int32, (256, 768), 0) % 16
    lanes = lax.broadcasted_iota(jnp.int32, (256, 768), 1) % 16
    mask = rows == lanes
    low = lax.broadcasted_iota(jnp.int32, (256, 128), 1) < 64

    def neighbour(axis, step):
        nx = (x + step * (1 - axis)) % 4
        nz = (z + step * axis) % 4
        return {"blk": nx * 4 + nz}

    def copies(s, kind, src, dst, axis):
        minus = pltpu.make_async_remote_copy(
            src_ref=src.at[s, 0], dst_ref=dst.at[s, 0], send_sem=s_sem.at[s, kind, 0], recv_sem=r_sem.at[s, kind, 0],
            device_id=neighbour(axis, 3), device_id_type=MESH)
        plus = pltpu.make_async_remote_copy(
            src_ref=src.at[s, 1], dst_ref=dst.at[s, 1], send_sem=s_sem.at[s, kind, 1], recv_sem=r_sem.at[s, kind, 1],
            device_id=neighbour(axis, 1), device_id_type=MESH)
        return minus, plus

    A, B = pl.ds(0, 128), pl.ds(128, 128)

    def compute(s):
        tt = s // 2
        par = s % 2
        qs = s % 4

        @pl.when(par == 0)
        def _():
            for h in (0, 1):
                t = tt + 4 * h
                pltpu.make_async_copy(leg_hbm.at[:, pl.ds(16 * t, 16), :], leg.at[t], leg_sem.at[t]).wait()

        lhs = []
        for h in (0, 1):
            sp = spec_ref[tt + 4 * h, pl.ds(16 * par, 16)]
            sp = sp.reshape(256, sp.shape[-1])
            ex = jnp.dot(sp, e_ref[...], preferred_element_type=F32)
            lhs.append(jnp.where(mask, ex, 0.0).astype(BF))
        for bx in range(4):
            pa, pb = [
                jnp.dot(lhs[h], leg[tt + 4 * h, :, :, 256 * bx:256 * bx + 256].reshape(768, 256),
                        preferred_element_type=F32)
                for h in (0, 1)
            ]
            for half in range(2):
                a = pa[:, 128 * half:128 * half + 128]
                b = pb[:, 128 * half:128 * half + 128]
                first = jnp.where(low, a, pltpu.roll(b, 64, 1))
                second = jnp.where(low, pltpu.roll(a, 64, 1), b)
                for bz, value in ((2 * half, first), (2 * half + 1, second)):
                    q[qs, bx * (1 - par) + bz * par, bz * (1 - par) + bx * par] = value
        i = x * (1 - par) + z * par
        c1, c2, c3 = (i + 1) % 4, (i + 2) % 4, (i + 3) % 4
        ms1[s, 0, 0] = q[qs, c2, :, A, :].astype(BF)
        ms1[s, 0, 1] = q[qs, c3, :, B, :].astype(BF)
        ms1[s, 1, 0] = q[qs, c2, :, B, :].astype(BF)
        ms1[s, 1, 1] = q[qs, c1, :, A, :].astype(BF)
        for c in copies(s, 0, ms1, mr1, par):
            c.start()

    def relay1(s):
        par = s % 2
        qs = s % 4
        i = x * (1 - par) + z * par
        c1, c3 = (i + 1) % 4, (i + 3) % 4
        minus, plus = copies(s, 0, ms1, mr1, par)
        send = copies(s, 1, ss1, sr1, par)
        minus.wait_recv()
        ss1[s, 0] = (q[qs, c3, :, A, :] + mr1[s, 0, 0].astype(F32)).astype(BF)
        send[0].start()
        plus.wait_recv()
        ss1[s, 1] = (q[qs, c1, :, B, :] + mr1[s, 1, 0].astype(F32)).astype(BF)
        send[1].start()

    def owner1(s):
        par = s % 2
        qs = s % 4
        i = x * (1 - par) + z * par
        minus, plus = copies(s, 1, ss1, sr1, par)
        minus.wait_recv()
        q2[s, :, A, :] = q[qs, i, :, A, :] + mr1[s, 1, 1].astype(F32) + sr1[s, 0].astype(F32)
        plus.wait_recv()
        q2[s, :, B, :] = q[qs, i, :, B, :] + mr1[s, 0, 1].astype(F32) + sr1[s, 1].astype(F32)
        j = z * (1 - par) + x * par
        d1, d2, d3 = (j + 1) % 4, (j + 2) % 4, (j + 3) % 4
        ms2[s, 0, 0] = q2[s, d2, A, :].astype(BF)
        ms2[s, 0, 1] = q2[s, d3, B, :].astype(BF)
        ms2[s, 1, 0] = q2[s, d2, B, :].astype(BF)
        ms2[s, 1, 1] = q2[s, d1, A, :].astype(BF)
        for c in copies(s, 2, ms2, mr2, 1 - par):
            c.start()

    def relay2(s):
        par = s % 2
        j = z * (1 - par) + x * par
        d1, d3 = (j + 1) % 4, (j + 3) % 4
        minus, plus = copies(s, 2, ms2, mr2, 1 - par)
        send = copies(s, 3, ss2, sr2, 1 - par)
        minus.wait_recv()
        ss2[s, 0] = (q2[s, d3, A, :] + mr2[s, 0, 0].astype(F32)).astype(BF)
        send[0].start()
        plus.wait_recv()
        ss2[s, 1] = (q2[s, d1, B, :] + mr2[s, 1, 0].astype(F32)).astype(BF)
        send[1].start()

    def owner2(s):
        par = s % 2
        j = z * (1 - par) + x * par
        minus, plus = copies(s, 3, ss2, sr2, 1 - par)
        minus.wait_recv()
        out_ref[s, A, :] = q2[s, j, A, :] + mr2[s, 1, 1].astype(F32) + sr2[s, 0].astype(F32)
        plus.wait_recv()
        out_ref[s, B, :] = q2[s, j, B, :] + mr2[s, 0, 1].astype(F32) + sr2[s, 1].astype(F32)

    stages = ((compute, 0), (relay1, 1), (owner1, 2), (relay2, 3), (owner2, 4))

    def step(k, carry):
        for stage, lag in stages:
            @pl.when((k >= lag) & (k < NBLOCK + lag))
            def _():
                stage(k - lag)
        return carry

    lax.fori_loop(0, NBLOCK + stages[-1][1], step, 0)

    def drain(s, carry):
        par = s % 2
        for kind, src, dst, axis in ((0, ms1, mr1, par), (1, ss1, sr1, par), (2, ms2, mr2, 1 - par), (3, ss2, sr2, 1 - par)):
            for c in copies(s, kind, src, dst, axis):
                c.wait_send()
        return carry

    lax.fori_loop(0, NBLOCK, drain, 0)


def contract(spec, expand, legendre):
    big = (NBLOCK, 2, 2, 4, 128, 128)
    small = (NBLOCK, 2, 2, 128, 128)
    vmem = pl.BlockSpec(memory_space=pltpu.VMEM)
    return pl.pallas_call(
        contract_kernel,
        out_shape=jax.ShapeDtypeStruct((NBLOCK, 256, 128), F32),
        in_specs=[vmem, vmem, pl.BlockSpec(memory_space=pl.ANY)],
        out_specs=vmem,
        scratch_shapes=[
            pltpu.VMEM((8, 48, 16, 1024), BF),
            pltpu.VMEM((4, 4, 4, 256, 128), F32),
            pltpu.VMEM((NBLOCK, 4, 256, 128), F32),
            pltpu.VMEM(big, BF), pltpu.VMEM(big, BF),
            pltpu.VMEM((NBLOCK, 2, 4, 128, 128), BF), pltpu.VMEM((NBLOCK, 2, 4, 128, 128), BF),
            pltpu.VMEM(small, BF), pltpu.VMEM(small, BF),
            pltpu.VMEM((NBLOCK, 2, 128, 128), BF), pltpu.VMEM((NBLOCK, 2, 128, 128), BF),
            pltpu.SemaphoreType.DMA((8,)),
            pltpu.SemaphoreType.DMA((NBLOCK, 4, 2)),
            pltpu.SemaphoreType.DMA((NBLOCK, 4, 2)),
        ],
        compiler_params=pltpu.CompilerParams(collective_id=0, has_side_effects=True, vmem_limit_bytes=60 * 2**20),
    )(spec, expand, legendre)


def finish(blocks):
    blocks = blocks.reshape(4, 2, 16, 16, 2, 64)
    return jnp.transpose(blocks, (5, 1, 2, 4, 0, 3)).reshape(64, 16, 2, 128)


def body(field, ocean_mask, plan, legendre):
    lon_local = field.shape[2]
    slot_dev = legendre.shape[0]
    masked = field * ocean_mask.astype(jnp.float32)[None]
    packed = pack_cycles(masked, plan, slot_dev)
    first = lax.axis_index("order") * lon_local
    terms = transform(packed, twiddle(first, lon_local))
    spectrum = lax.psum_scatter(terms, "order", scatter_dimension=3, tiled=True).astype(
        jnp.bfloat16
    )
    spec = spectrum.reshape(16, 48, 2, 8, 16).transpose(3, 0, 2, 4, 1).reshape(8, 32, 16, 48)
    slots = jnp.arange(48, dtype=jnp.int32)[:, None]
    expand = (slots == jnp.arange(768, dtype=jnp.int32)[None, :] // 16).astype(BF)
    return finish(contract(spec, expand, legendre))


def solution(mesh):
    placed = (P(None, "blk", "order"), P("blk", "order"), P(), P("blk", "order", None))
    return jax.shard_map(
        body, mesh=mesh, in_specs=placed, out_specs=P("blk", None, None, "order"), check_vma=False
    )
```

```python
import math

import jax
import jax.numpy as jnp
import numpy as np
from jax import lax
from jax.experimental import pallas as pl
from jax.experimental.pallas import tpu as pltpu
from jax.sharding import PartitionSpec as P

NLON = 4096
MESH = pl.DeviceIdType.MESH
BF = jnp.bfloat16
F32 = jnp.float32
NBLOCK = 8


def dft_tables():
    r = np.arange(16)[:, None, None]
    column = np.arange(128)[None, :, None]
    owner, w, c, ql = column // 16, column // 8 % 2, column // 4 % 2, column % 4
    residue = np.where(w == 0, r, np.where(r == 0, 16, 32 - r))
    m = 32 * (4 * owner + ql) + residue
    i = np.arange(128)[None, None, :]
    angle = 2.0 * np.pi * (m * i % NLON) / NLON
    cos, sin = np.cos(angle) / 64.0, np.sin(angle) / 64.0
    real = np.where(c == 0, cos, -sin)
    imag = np.where(c == 0, sin, cos)
    imag = np.where(w == 0, imag, -imag)
    real, imag = (
        np.where((r == 0) & (w == 1), 0.0, real),
        np.where(r == 0, np.where(w == 1, np.where(c == 0, cos, -sin), 0.0), imag),
    )
    table = np.concatenate([real, imag], axis=2).astype(np.float32)
    high = table.astype(jnp.bfloat16)
    low = (table - high.astype(np.float32)).astype(jnp.bfloat16)
    return high, low


def order_permutation():
    out = np.zeros((256, 256), np.float32)
    for r in range(16):
        for w in range(2):
            for c in range(2):
                for ql in range(4):
                    m = r if w == 0 else (16 - r) % 16
                    out[(2 * ql + w) * 32 + c * 16 + m, r * 16 + w * 8 + c * 4 + ql] = 1.0
    return out.astype(jnp.bfloat16)


def real_dft(values):
    n = len(values)
    if n == 2:
        return [(values[0] + values[1], None), (values[0] - values[1], None)]
    even, odd = real_dft(values[0::2]), real_dft(values[1::2])
    half = n // 2

    def term(part, k):
        if k <= half // 2:
            return part[k]
        re, im = part[half - k]
        return re, (None if im is None else -im)

    result = [None] * (half + 1)
    for k in range(half // 2 + 1):
        er, ei = even[k]
        qr, qi = odd[k]
        cos, sin = math.cos(2 * math.pi * k / n), math.sin(2 * math.pi * k / n)
        if k == 0:
            result[0] = (er + qr, None)
            result[half] = (er - qr, None)
            continue
        if 4 * k == n:
            tr, ti = qi, -qr
        else:
            tr = qr * cos + qi * sin if qi is not None else qr * cos
            ti = qi * cos - qr * sin if qi is not None else -(qr * sin)

        def add(a, b, sign):
            if a is None:
                return None if b is None else (b if sign > 0 else -b)
            if b is None:
                return a
            return a + b if sign > 0 else a - b

        result[k] = (add(er, tr, 1), add(ei, ti, 1))
        if k != half - k:
            ni = add(ei, ti, -1)
            result[half - k] = (add(er, tr, -1), None if ni is None else -ni)
    return result


def spectrum_kernel(field_ref, mask_ref, high_ref, low_ref, perm_ref, place_ref, out_ref,
                    masked, xr, relay, ycat, terms, sbuf, srecv,
                    far_s, far_r, near_s, near_r, fwd_s, fwd_r, side_s, side_r, ex_s, ex_r):
    me = lax.axis_index("order")
    y = me // 2
    core = me % 2
    barrier = pltpu.get_barrier_semaphore()
    peers = [(dy, dc) for dy in range(4) for dc in range(2) if (dy, dc) != (0, 0)]

    def at(dy, other):
        return {"order": (y + dy) % 4 * 2 + other}

    for dy, dc in peers:
        pl.semaphore_signal(barrier, inc=1, device_id=at(dy, (core + dc) % 2), device_id_type=MESH)

    ocean = mask_ref[...].astype(F32)

    def mask_field(f, carry):
        masked[f] = field_ref[f] * ocean
        return carry

    lax.fori_loop(0, 16, mask_field, 0)
    pl.semaphore_wait(barrier, 7)

    halves = (pl.ds(0, 32), pl.ds(32, 32))
    steps = (1, 3)

    def remote(src, dst, ss, rs, device):
        return pltpu.make_async_remote_copy(src_ref=src, dst_ref=dst, send_sem=ss, recv_sem=rs,
                                            device_id=device, device_id_type=MESH)

    def far(g, d, other):
        target = ((y + 2) % 4 * 2 + other) * 2 + g
        return remote(masked.at[target, halves[d]], relay.at[g, d, core], far_s.at[g, d, other], far_r.at[g, d, core],
                      at(steps[d], other))

    def near(g, d, other):
        target = ((y + steps[d]) % 4 * 2 + other) * 2 + g
        return remote(masked.at[target], xr.at[g, me], near_s.at[g, d, other], near_r.at[g, d, core],
                      at(steps[d], other))

    def forward(g, d, source):
        origin = (y + 4 - steps[d]) % 4 * 2 + source
        return remote(relay.at[g, d, source], xr.at[g, origin, halves[d]], fwd_s.at[g, d, source], fwd_r.at[g, d, source],
                      at(steps[d], core))

    def side(g):
        target = (y * 2 + 1 - core) * 2 + g
        return remote(masked.at[target], xr.at[g, me], side_s.at[g], side_r.at[g], at(0, 1 - core))

    def wait_far(g, d, source):
        remote(masked.at[0, halves[d]], relay.at[g, d, source], far_s.at[g, d, source], far_r.at[g, d, source],
               at(steps[d], source)).wait_recv()

    def wait_near(g, d, source):
        remote(masked.at[0], xr.at[g, me], near_s.at[g, d, source], near_r.at[g, d, source],
               at(steps[d], source)).wait_recv()

    for g in range(2):
        for d in range(2):
            for other in range(2):
                far(g, d, other).start()
        for d in range(2):
            for other in range(2):
                near(g, d, other).start()
        side(g).start()
    for g in range(2):
        xr[g, me] = masked[me * 2 + g]

    for g in range(2):
        for d in range(2):
            for source in range(2):
                wait_far(g, d, source)
                forward(g, d, source).start()
    for g in range(2):
        for d in range(2):
            for source in range(2):
                wait_near(g, d, source)
        side(g).wait_recv()
        for d in range(2):
            for source in range(2):
                forward(g, d, source).wait_recv()

        def butterfly(k, carry):
            rows = pl.ds(pl.multiple_of(16 * k, 16), 16)
            values = [xr[g, a // 4, rows, 128 * (a % 4):128 * (a % 4) + 128] for a in range(32)]
            result = real_dft(values)
            out_rows = pl.ds(pl.multiple_of(64 * g + 16 * k, 16), 16)
            for r in range(16):
                pair = (result[0][0], result[16][0]) if r == 0 else result[r]
                for part, value in enumerate(pair):
                    high = value.astype(BF)
                    ycat[r, out_rows, 128 * part:128 * part + 128] = high
                    ycat[r, out_rows, 256 + 128 * part:384 + 128 * part] = (value - high.astype(F32)).astype(BF)
            return carry

        lax.fori_loop(0, 4, butterfly, 0)

    contract_lanes = (((1,), (1,)), ((), ()))

    def transform(r, carry):
        yh, yl = ycat[r, :, 0:256], ycat[r, :, 256:512]
        th, tl = high_ref[r], low_ref[r]
        out = lax.dot_general(th, yh, contract_lanes, preferred_element_type=F32)
        out += lax.dot_general(th, yl, contract_lanes, preferred_element_type=F32)
        out += lax.dot_general(tl, yh, contract_lanes, preferred_element_type=F32)
        terms[:, r] = out.astype(BF).reshape(8, 16, 128)
        return carry

    lax.fori_loop(0, 16, transform, 0)

    def arrange(o, carry):
        part = jnp.dot(perm_ref[...], terms[o].reshape(256, 128), preferred_element_type=F32)
        sbuf[o] = part.astype(BF).reshape(8, 32, 128)
        return carry

    lax.fori_loop(0, 8, arrange, 0)

    def exchange(dy, dc):
        target = (y + dy) % 4 * 2 + (core + dc) % 2
        return remote(sbuf.at[target], srecv.at[me], ex_s.at[dy, dc], ex_r.at[dy, dc], {"order": target})

    for dy, dc in peers:
        exchange(dy, dc).start()
    srecv[me] = sbuf[me]
    for dy, dc in peers:
        exchange(dy, dc).wait_recv()

    def place(tt, carry):
        parts = []
        for h in range(2):
            rows = srecv[:, tt + 4 * h].reshape(256, 128)
            out = lax.dot_general(place_ref[...], rows, contract_lanes, preferred_element_type=F32)
            parts.append(out.reshape(16, 8, 256))
        out_ref[:, tt] = jnp.concatenate(parts, axis=1).astype(BF)
        return carry

    lax.fori_loop(0, 4, place, 0)

    for g in range(2):
        for d in range(2):
            for other in range(2):
                far(g, d, other).wait_send()
                near(g, d, other).wait_send()
                forward(g, d, other).wait_send()
        side(g).wait_send()
    for dy, dc in peers:
        exchange(dy, dc).wait_send()


def spectrum_blocks(field, mask, place):
    high, low = dft_tables()
    vmem = pl.BlockSpec(memory_space=pltpu.VMEM)
    dma = pltpu.SemaphoreType.DMA
    return pl.pallas_call(
        spectrum_kernel,
        out_shape=jax.ShapeDtypeStruct((16, 4, 16, 256), BF),
        in_specs=[vmem] * 6,
        out_specs=vmem,
        scratch_shapes=[
            pltpu.VMEM((16, 64, 512), F32),
            pltpu.VMEM((2, 8, 64, 512), F32),
            pltpu.VMEM((2, 2, 2, 32, 512), F32),
            pltpu.VMEM((16, 128, 512), BF),
            pltpu.VMEM((8, 16, 16, 128), BF),
            pltpu.VMEM((8, 8, 32, 128), BF),
            pltpu.VMEM((8, 8, 32, 128), BF),
            dma((2, 2, 2)), dma((2, 2, 2)), dma((2, 2, 2)), dma((2, 2, 2)), dma((2, 2, 2)), dma((2, 2, 2)),
            dma((2,)), dma((2,)), dma((4, 2)), dma((4, 2)),
        ],
        compiler_params=pltpu.CompilerParams(collective_id=1, has_side_effects=True, vmem_limit_bytes=40 * 2**20),
    )(field, mask, jnp.asarray(high), jnp.asarray(low), jnp.asarray(order_permutation()), place)


def plan_maps(plan):
    own = lax.axis_index("blk")
    grid = plan.reshape(16, 64)
    owner = grid // 48
    positions = jnp.arange(64, dtype=jnp.int32)
    earlier = positions[None, :] < positions[:, None]
    rank = jnp.sum((owner[:, :, None] == owner[:, None, :]) & earlier[None], axis=2, dtype=jnp.int32)
    own_owner = lax.dynamic_index_in_dim(owner, own, 0, keepdims=False)
    own_rank = lax.dynamic_index_in_dim(rank, own, 0, keepdims=False)
    row = jnp.arange(128, dtype=jnp.int32)[:, None]
    match = (own_owner[None, :] == row // 8) & (own_rank[None, :] == row // 2 % 4)
    place = jnp.concatenate([match & (row % 2 == 0), match & (row % 2 == 1)], axis=1).astype(BF)
    ranks = jnp.arange(4, dtype=jnp.int32)
    to_rank = ((rank[:, None, :] == ranks[None, :, None]) & (owner == own)[:, None, :]).astype(BF)
    to_slot = ((grid % 48)[:, :, None] == jnp.arange(768, dtype=jnp.int32)[None, None, :] // 16).astype(BF)
    expand = jnp.einsum("brc,bcp->brp", to_rank, to_slot, preferred_element_type=F32).astype(BF)
    expand = jnp.broadcast_to(expand[:, None, :, None, :], (16, 2, 4, 2, 768)).reshape(256, 768)
    return place, expand


def contract_kernel(sent_ref, e_ref, leg_hbm, out_ref, arrived, leg, q, q2, ms1, mr1, ss1, sr1, ms2, mr2, ss2, sr2,
                    leg_sem, ex_s, ex_r, s_sem, r_sem):
    me = lax.axis_index("blk")
    x = me // 4
    z = me % 4
    for t in range(8):
        pltpu.make_async_copy(leg_hbm.at[:, pl.ds(16 * t, 16), :], leg.at[t], leg_sem.at[t]).start()
    barrier = pltpu.get_barrier_semaphore()
    peers = [(dx, dz) for dx in range(4) for dz in range(4) if (dx, dz) != (0, 0)]
    for dx, dz in peers:
        pl.semaphore_signal(barrier, inc=1, device_id={"blk": (x + dx) % 4 * 4 + (z + dz) % 4}, device_id_type=MESH)
    pl.semaphore_wait(barrier, 15)

    def exchange(dx, dz):
        target = (x + dx) % 4 * 4 + (z + dz) % 4
        return pltpu.make_async_remote_copy(
            src_ref=sent_ref.at[target], dst_ref=arrived.at[me], send_sem=ex_s.at[dx, dz], recv_sem=ex_r.at[dx, dz],
            device_id={"blk": target}, device_id_type=MESH)

    for dx, dz in peers:
        exchange(dx, dz).start()
    arrived[me] = sent_ref[me]
    for dx, dz in peers:
        exchange(dx, dz).wait_recv()

    rows = lax.broadcasted_iota(jnp.int32, (256, 768), 0) % 16
    lanes = lax.broadcasted_iota(jnp.int32, (256, 768), 1) % 16
    mask = rows == lanes
    place = lax.broadcasted_iota(jnp.int32, (256, 768), 0)
    low = lax.broadcasted_iota(jnp.int32, (256, 128), 1) < 64

    def neighbour(axis, step):
        nx = (x + step * (1 - axis)) % 4
        nz = (z + step * axis) % 4
        return {"blk": nx * 4 + nz}

    def copies(s, kind, src, dst, axis):
        minus = pltpu.make_async_remote_copy(
            src_ref=src.at[s, 0], dst_ref=dst.at[s, 0], send_sem=s_sem.at[s, kind, 0], recv_sem=r_sem.at[s, kind, 0],
            device_id=neighbour(axis, 3), device_id_type=MESH)
        plus = pltpu.make_async_remote_copy(
            src_ref=src.at[s, 1], dst_ref=dst.at[s, 1], send_sem=s_sem.at[s, kind, 1], recv_sem=r_sem.at[s, kind, 1],
            device_id=neighbour(axis, 1), device_id_type=MESH)
        return minus, plus

    A, B = pl.ds(0, 128), pl.ds(128, 128)

    def compute(s):
        tt = s // 2
        par = s % 2
        qs = s % 4

        @pl.when(par == 0)
        def _():
            for h in (0, 1):
                t = tt + 4 * h
                pltpu.make_async_copy(leg_hbm.at[:, pl.ds(16 * t, 16), :], leg.at[t], leg_sem.at[t]).wait()

        lhs = []
        values = arrived[:, tt].reshape(256, 256)
        for h in (0, 1):
            expand = jnp.where((place // 8 % 2 == h) & (place % 2 == par), e_ref[...].astype(F32), 0.0).astype(BF)
            ex = lax.dot_general(values, expand, (((0,), (0,)), ((), ())), preferred_element_type=F32)
            lhs.append(jnp.where(mask, ex, 0.0).astype(BF))
        for bx in range(4):
            pa, pb = [
                jnp.dot(lhs[h], leg[tt + 4 * h, :, :, 256 * bx:256 * bx + 256].reshape(768, 256),
                        preferred_element_type=F32)
                for h in (0, 1)
            ]
            for half in range(2):
                a = pa[:, 128 * half:128 * half + 128]
                b = pb[:, 128 * half:128 * half + 128]
                first = jnp.where(low, a, pltpu.roll(b, 64, 1))
                second = jnp.where(low, pltpu.roll(a, 64, 1), b)
                for bz, value in ((2 * half, first), (2 * half + 1, second)):
                    q[qs, bx * (1 - par) + bz * par, bz * (1 - par) + bx * par] = value
        i = x * (1 - par) + z * par
        c1, c2, c3 = (i + 1) % 4, (i + 2) % 4, (i + 3) % 4
        ms1[s, 0, 0] = q[qs, c2, :, A, :].astype(BF)
        ms1[s, 0, 1] = q[qs, c3, :, B, :].astype(BF)
        ms1[s, 1, 0] = q[qs, c2, :, B, :].astype(BF)
        ms1[s, 1, 1] = q[qs, c1, :, A, :].astype(BF)
        for c in copies(s, 0, ms1, mr1, par):
            c.start()

    def relay1(s):
        par = s % 2
        qs = s % 4
        i = x * (1 - par) + z * par
        c1, c3 = (i + 1) % 4, (i + 3) % 4
        minus, plus = copies(s, 0, ms1, mr1, par)
        send = copies(s, 1, ss1, sr1, par)
        minus.wait_recv()
        ss1[s, 0] = (q[qs, c3, :, A, :] + mr1[s, 0, 0].astype(F32)).astype(BF)
        send[0].start()
        plus.wait_recv()
        ss1[s, 1] = (q[qs, c1, :, B, :] + mr1[s, 1, 0].astype(F32)).astype(BF)
        send[1].start()

    def owner1(s):
        par = s % 2
        qs = s % 4
        i = x * (1 - par) + z * par
        minus, plus = copies(s, 1, ss1, sr1, par)
        minus.wait_recv()
        q2[s, :, A, :] = q[qs, i, :, A, :] + mr1[s, 1, 1].astype(F32) + sr1[s, 0].astype(F32)
        plus.wait_recv()
        q2[s, :, B, :] = q[qs, i, :, B, :] + mr1[s, 0, 1].astype(F32) + sr1[s, 1].astype(F32)
        j = z * (1 - par) + x * par
        d1, d2, d3 = (j + 1) % 4, (j + 2) % 4, (j + 3) % 4
        ms2[s, 0, 0] = q2[s, d2, A, :].astype(BF)
        ms2[s, 0, 1] = q2[s, d3, B, :].astype(BF)
        ms2[s, 1, 0] = q2[s, d2, B, :].astype(BF)
        ms2[s, 1, 1] = q2[s, d1, A, :].astype(BF)
        for c in copies(s, 2, ms2, mr2, 1 - par):
            c.start()

    def relay2(s):
        par = s % 2
        j = z * (1 - par) + x * par
        d1, d3 = (j + 1) % 4, (j + 3) % 4
        minus, plus = copies(s, 2, ms2, mr2, 1 - par)
        send = copies(s, 3, ss2, sr2, 1 - par)
        minus.wait_recv()
        ss2[s, 0] = (q2[s, d3, A, :] + mr2[s, 0, 0].astype(F32)).astype(BF)
        send[0].start()
        plus.wait_recv()
        ss2[s, 1] = (q2[s, d1, B, :] + mr2[s, 1, 0].astype(F32)).astype(BF)
        send[1].start()

    def owner2(s):
        par = s % 2
        j = z * (1 - par) + x * par
        minus, plus = copies(s, 3, ss2, sr2, 1 - par)
        minus.wait_recv()
        out_ref[s, A, :] = q2[s, j, A, :] + mr2[s, 1, 1].astype(F32) + sr2[s, 0].astype(F32)
        plus.wait_recv()
        out_ref[s, B, :] = q2[s, j, B, :] + mr2[s, 0, 1].astype(F32) + sr2[s, 1].astype(F32)

    stages = ((compute, 0), (relay1, 1), (owner1, 2), (relay2, 3), (owner2, 4))

    def step(k, carry):
        for stage, lag in stages:
            @pl.when((k >= lag) & (k < NBLOCK + lag))
            def _():
                stage(k - lag)
        return carry

    lax.fori_loop(0, NBLOCK + stages[-1][1], step, 0)

    def drain(s, carry):
        par = s % 2
        for kind, src, dst, axis in ((0, ms1, mr1, par), (1, ss1, sr1, par), (2, ms2, mr2, 1 - par), (3, ss2, sr2, 1 - par)):
            for c in copies(s, kind, src, dst, axis):
                c.wait_send()
        return carry

    lax.fori_loop(0, NBLOCK, drain, 0)
    for dx, dz in peers:
        exchange(dx, dz).wait_send()


def contract(sent, expand, legendre):
    big = (NBLOCK, 2, 2, 4, 128, 128)
    small = (NBLOCK, 2, 2, 128, 128)
    vmem = pl.BlockSpec(memory_space=pltpu.VMEM)
    return pl.pallas_call(
        contract_kernel,
        out_shape=jax.ShapeDtypeStruct((NBLOCK, 256, 128), F32),
        in_specs=[vmem, vmem, pl.BlockSpec(memory_space=pl.ANY)],
        out_specs=vmem,
        scratch_shapes=[
            pltpu.VMEM((16, 4, 16, 256), BF),
            pltpu.VMEM((8, 48, 16, 1024), BF),
            pltpu.VMEM((4, 4, 4, 256, 128), F32),
            pltpu.VMEM((NBLOCK, 4, 256, 128), F32),
            pltpu.VMEM(big, BF), pltpu.VMEM(big, BF),
            pltpu.VMEM((NBLOCK, 2, 4, 128, 128), BF), pltpu.VMEM((NBLOCK, 2, 4, 128, 128), BF),
            pltpu.VMEM(small, BF), pltpu.VMEM(small, BF),
            pltpu.VMEM((NBLOCK, 2, 128, 128), BF), pltpu.VMEM((NBLOCK, 2, 128, 128), BF),
            pltpu.SemaphoreType.DMA((8,)),
            pltpu.SemaphoreType.DMA((4, 4)),
            pltpu.SemaphoreType.DMA((4, 4)),
            pltpu.SemaphoreType.DMA((NBLOCK, 4, 2)),
            pltpu.SemaphoreType.DMA((NBLOCK, 4, 2)),
        ],
        compiler_params=pltpu.CompilerParams(collective_id=0, has_side_effects=True, vmem_limit_bytes=60 * 2**20),
    )(sent, expand, legendre)


def finish(blocks):
    blocks = blocks.reshape(4, 2, 8, 2, 16, 2, 64)
    return jnp.transpose(blocks, (6, 2, 1, 3, 5, 0, 4)).reshape(64, 16, 2, 128)


def body(field, ocean_mask, plan, legendre):
    place, expand = plan_maps(plan)
    sent = spectrum_blocks(field, ocean_mask, place)
    return finish(contract(sent, expand, legendre))


def solution(mesh):
    placed = (P(None, "blk", "order"), P("blk", "order"), P(), P("blk", "order", None))
    return jax.shard_map(
        body, mesh=mesh, in_specs=placed, out_specs=P("blk", None, None, "order"), check_vma=False
    )
```

```python
import math

import jax
import jax.numpy as jnp
import numpy as np
from jax import lax
from jax.experimental import pallas as pl
from jax.experimental.pallas import tpu as pltpu
from jax.sharding import PartitionSpec as P

NLON = 4096
MESH = pl.DeviceIdType.MESH
BF = jnp.bfloat16
F32 = jnp.float32
NBLOCK = 8
CONTRACT_LANES = (((1,), (1,)), ((), ()))
CONTRACT_ROWS = (((0,), (0,)), ((), ()))

STEP_A, STEP_B, STEP_C, DELAY = 7, 8, 11, 4
LAGS = (0, 4, 6, 8, 10)
FIRST = 3


def dft_tables():
    r = np.arange(16)[:, None, None]
    column = np.arange(128)[None, :, None]
    owner, w, c, ql = column // 16, column // 8 % 2, column // 4 % 2, column % 4
    residue = np.where(w == 0, r, np.where(r == 0, 16, 32 - r))
    m = 32 * (4 * owner + ql) + residue
    i = np.arange(128)[None, None, :]
    angle = 2.0 * np.pi * (m * i % NLON) / NLON
    cos, sin = np.cos(angle) / 64.0, np.sin(angle) / 64.0
    real = np.where(c == 0, cos, -sin)
    imag = np.where(c == 0, sin, cos)
    imag = np.where(w == 0, imag, -imag)
    real, imag = (
        np.where((r == 0) & (w == 1), 0.0, real),
        np.where(r == 0, np.where(w == 1, np.where(c == 0, cos, -sin), 0.0), imag),
    )
    table = np.concatenate([real, imag], axis=2).astype(np.float32)
    high = table.astype(jnp.bfloat16)
    low = (table - high.astype(np.float32)).astype(jnp.bfloat16)
    return high, low


def order_permutation():
    out = np.zeros((128, 128), np.float32)
    for r in range(8):
        for w in range(2):
            for c in range(2):
                for ql in range(4):
                    mh = r if w == 0 else (8 - r) % 8
                    out[(2 * ql + w) * 16 + c * 8 + mh, r * 16 + w * 8 + c * 4 + ql] = 1.0
    return out.astype(jnp.bfloat16)


def real_dft(values):
    n = len(values)
    if n == 2:
        return [(values[0] + values[1], None), (values[0] - values[1], None)]
    even, odd = real_dft(values[0::2]), real_dft(values[1::2])
    half = n // 2

    def term(part, k):
        if k <= half // 2:
            return part[k]
        re, im = part[half - k]
        return re, (None if im is None else -im)

    result = [None] * (half + 1)
    for k in range(half // 2 + 1):
        er, ei = even[k]
        qr, qi = odd[k]
        cos, sin = math.cos(2 * math.pi * k / n), math.sin(2 * math.pi * k / n)
        if k == 0:
            result[0] = (er + qr, None)
            result[half] = (er - qr, None)
            continue
        if 4 * k == n:
            tr, ti = qi, -qr
        else:
            tr = qr * cos + qi * sin if qi is not None else qr * cos
            ti = qi * cos - qr * sin if qi is not None else -(qr * sin)

        def add(a, b, sign):
            if a is None:
                return None if b is None else (b if sign > 0 else -b)
            if b is None:
                return a
            return a + b if sign > 0 else a - b

        result[k] = (add(er, tr, 1), add(ei, ti, 1))
        if k != half - k:
            ni = add(ei, ti, -1)
            result[half - k] = (add(er, tr, -1), None if ni is None else -ni)
    return result


def kernel(field_hbm, mask_hbm, plan_ref, high_hbm, low_hbm, perm_hbm, leg_hbm, out_ref,
           masked, mask, high, low, perm, xr, relay, ycat, terms, sbuf, srecv, place, expand, sent, arrived,
           leg, q, q2, ms1, mr1, ss1, sr1, ms2, mr2, ss2, sr2, final,
           field_sem, load_sem, leg_sem, far_s, far_r, near_s, near_r, fwd_s, fwd_r, side_s, side_r,
           ox_s, ox_r, bx_s, bx_r, ring_s, ring_r):
    order = lax.axis_index("order")
    y, core = order // 2, order % 2
    me = lax.axis_index("blk")
    x, z = me // 4, me % 4

    def load_field(g, o):
        f = 2 * o + g
        return pltpu.make_async_copy(field_hbm.at[f], masked.at[f], field_sem.at[f])

    loads = [pltpu.make_async_copy(src, dst, load_sem.at[i]) for i, (src, dst) in enumerate(
        ((mask_hbm, mask), (high_hbm, high), (low_hbm, low), (perm_hbm, perm)))]

    def load_leg(t):
        return pltpu.make_async_copy(leg_hbm.at[:, pl.ds(16 * t, 16), :], leg.at[t], leg_sem.at[t])

    loads[0].start()
    for g in range(2):
        for o in range(8):
            load_field(g, o).start()
    for copy in loads[1:]:
        copy.start()
    for t in range(8):
        load_leg(t).start()

    barrier = pltpu.get_barrier_semaphore()
    order_peers = [(dy, dc) for dy in range(4) for dc in range(2) if (dy, dc) != (0, 0)]
    blk_peers = [(dx, dz) for dx in range(4) for dz in range(4) if (dx, dz) != (0, 0)]

    def at(dy, other):
        return {"order": (y + dy) % 4 * 2 + other}

    for dy, dc in order_peers:
        pl.semaphore_signal(barrier, inc=1, device_id=at(dy, (core + dc) % 2), device_id_type=MESH)
    for dx, dz in blk_peers:
        pl.semaphore_signal(barrier, inc=1, device_id={"blk": (x + dx) % 4 * 4 + (z + dz) % 4}, device_id_type=MESH)

    loads[0].wait()

    def mask_fields(g):
        for o in range(8):
            load_field(g, o).wait()

        def one(o, carry):
            masked[2 * o + g] = masked[2 * o + g] * mask[...].astype(F32)
            return carry

        lax.fori_loop(0, 8, one, 0)
        xr[g, order] = masked[order * 2 + g]

    def remote(src, dst, ss, rs, device):
        return pltpu.make_async_remote_copy(src_ref=src, dst_ref=dst, send_sem=ss, recv_sem=rs,
                                            device_id=device, device_id_type=MESH)

    halves = (pl.ds(0, 32), pl.ds(32, 32))
    steps = (1, 3)
    pairs = [(d, other) for d in range(2) for other in range(2)]

    def far(g, d, other):
        target = ((y + 2) % 4 * 2 + other) * 2 + g
        return remote(masked.at[target, halves[d]], relay.at[g, d, core], far_s.at[g, d, other], far_r.at[g, d, core],
                      at(steps[d], other))

    def near(g, d, other):
        target = ((y + steps[d]) % 4 * 2 + other) * 2 + g
        return remote(masked.at[target], xr.at[g, order], near_s.at[g, d, other], near_r.at[g, d, core],
                      at(steps[d], other))

    def forward(g, d, source):
        origin = (y + 4 - steps[d]) % 4 * 2 + source
        return remote(relay.at[g, d, source], xr.at[g, origin, halves[d]], fwd_s.at[g, d, source], fwd_r.at[g, d, source],
                      at(steps[d], core))

    def side(g):
        target = (y * 2 + 1 - core) * 2 + g
        return remote(masked.at[target], xr.at[g, order], side_s.at[g], side_r.at[g], at(0, 1 - core))

    def wait_far(g, d, source):
        remote(masked.at[0, halves[d]], relay.at[g, d, source], far_s.at[g, d, source], far_r.at[g, d, source],
               at(steps[d], source)).wait_recv()

    def wait_near(g, d, source):
        remote(masked.at[0], xr.at[g, order], near_s.at[g, d, source], near_r.at[g, d, source],
               at(steps[d], source)).wait_recv()

    mask_fields(0)
    pl.semaphore_wait(barrier, 22)
    for d, other in pairs:
        far(0, d, other).start()
    for d, other in pairs:
        near(0, d, other).start()
    side(0).start()
    mask_fields(1)
    for d, other in pairs:
        far(1, d, other).start()
    side(1).start()

    earlier = (lax.broadcasted_iota(jnp.int32, (64, 64), 0) < lax.broadcasted_iota(jnp.int32, (64, 64), 1))
    earlier = earlier.astype(F32).astype(BF)

    def owner_of(slots, rows):
        slots = jnp.broadcast_to(slots, (rows, 64))
        owner = jnp.zeros((rows, 64), jnp.int32)
        for b in range(1, 17):
            owner += (slots >= 48 * b).astype(jnp.int32)
        return slots, owner

    row = lax.broadcasted_iota(jnp.int32, (128, 64), 0)
    _, owner = owner_of(plan_ref[pl.ds(me, 1), :], 128)
    mine = owner == row // 8
    count = jnp.dot(mine.astype(F32).astype(BF), earlier, preferred_element_type=F32)
    match = mine & (count == (row // 2 % 4).astype(F32))
    for rh in range(2):
        place[:, 64 * rh:64 * rh + 64] = (match & (row % 2 == rh)).astype(F32).astype(BF)

    def source_map(b, carry):
        slots, owner = owner_of(plan_ref[pl.ds(b, 1), :], 16)
        mine = owner == me
        count = jnp.dot(mine.astype(F32).astype(BF), earlier, preferred_element_type=F32)
        rows = lax.broadcasted_iota(jnp.int32, (16, 64), 0)
        match = mine & (count == (rows // 2 % 4).astype(F32))
        slot = jnp.sum(jnp.where(match, (slots - 48 * me + 1).astype(F32), 0.0), axis=1, keepdims=True)
        lanes = lax.broadcasted_iota(jnp.int32, (16, 768), 1) // 16 + 1
        rows = lax.broadcasted_iota(jnp.int32, (16, 768), 0)
        hit = jnp.broadcast_to(slot, (16, 768)) == lanes.astype(F32)
        for h in range(2):
            for rh in range(2):
                expand[h, rh, pl.ds(pl.multiple_of(16 * b, 16), 16), :] = (
                    hit & (rows // 8 == h) & (rows % 2 == rh)).astype(F32).astype(BF)
        return carry

    lax.fori_loop(0, 16, source_map, 0)
    for copy in loads[1:]:
        copy.wait()

    def exchange_order(g, dy, dc):
        target = (y + dy) % 4 * 2 + (core + dc) % 2
        return remote(sbuf.at[g, target], srecv.at[g, order], ox_s.at[g, dy, dc], ox_r.at[g, dy, dc], {"order": target})

    def exchange_blk(g, dx, dz):
        target = (x + dx) % 4 * 4 + (z + dz) % 4
        return remote(sent.at[g, target], arrived.at[g, me], bx_s.at[g, dx, dz], bx_r.at[g, dx, dz], {"blk": target})

    def pass_on(g):
        for d, source in pairs:
            wait_far(g, d, source)
            forward(g, d, source).start()

    def transform_group(g):
        for d, source in pairs:
            wait_near(g, d, source)
        side(g).wait_recv()
        for d, source in pairs:
            forward(g, d, source).wait_recv()

        def butterfly(k, carry):
            rows = pl.ds(pl.multiple_of(16 * k, 16), 16)
            values = [xr[g, a // 4, rows, 128 * (a % 4):128 * (a % 4) + 128] for a in range(32)]
            result = real_dft(values)
            for r in range(16):
                pair = (result[0][0], result[16][0]) if r == 0 else result[r]
                for part, value in enumerate(pair):
                    top = value.astype(BF)
                    ycat[r, rows, 128 * part:128 * part + 128] = top
                    ycat[r, rows, 256 + 128 * part:384 + 128 * part] = (value - top.astype(F32)).astype(BF)
            return carry

        lax.fori_loop(0, 4, butterfly, 0)

        def transform(r, carry):
            parts = []
            for rr in (r, r + 8):
                yh, yl = ycat[rr, :, 0:256], ycat[rr, :, 256:512]
                out = lax.dot_general(high[rr], yh, CONTRACT_LANES, preferred_element_type=F32)
                out += lax.dot_general(high[rr], yl, CONTRACT_LANES, preferred_element_type=F32)
                out += lax.dot_general(low[rr], yh, CONTRACT_LANES, preferred_element_type=F32)
                parts.append(out)
            terms[:, r] = jnp.concatenate(parts, axis=1).astype(BF).reshape(8, 16, 128)
            return carry

        lax.fori_loop(0, 8, transform, 0)

        def arrange(o, carry):
            part = jnp.dot(perm[...], terms[o].reshape(128, 128), preferred_element_type=F32)
            sbuf[g, o] = part.astype(BF).reshape(8, 16, 128)
            return carry

        lax.fori_loop(0, 8, arrange, 0)
        for dy, dc in order_peers:
            exchange_order(g, dy, dc).start()
        srecv[g, order] = sbuf[g, order]

    def place_group(g):
        for dy, dc in order_peers:
            exchange_order(g, dy, dc).wait_recv()
        for tt in range(4):
            parts = []
            for h in range(2):
                rows = srecv[g, :, tt + 4 * h].reshape(128, 128)
                out = lax.dot_general(place[...], rows, CONTRACT_LANES, preferred_element_type=F32)
                parts.append(out.reshape(16, 8, 128))
            sent[g, :, tt] = jnp.concatenate(parts, axis=1).astype(BF)
        for dx, dz in blk_peers:
            exchange_blk(g, dx, dz).start()
        arrived[g, me] = sent[g, me]

    def receive_group(g):
        for dx, dz in blk_peers:
            exchange_blk(g, dx, dz).wait_recv()

    low_lanes = lax.broadcasted_iota(jnp.int32, (256, 128), 1) < 64

    def neighbour(axis, step):
        nx = (x + step * (1 - axis)) % 4
        nz = (z + step * axis) % 4
        return {"blk": nx * 4 + nz}

    def copies(s, kind, src, dst, axis):
        return [remote(src.at[s, way], dst.at[s, way], ring_s.at[s, kind, way], ring_r.at[s, kind, way],
                       neighbour(axis, 3 - 2 * way)) for way in range(2)]

    A, B = pl.ds(0, 128), pl.ds(128, 128)

    def compute(s):
        g, tt, par, qs = s // 4, s % 4, s % 2, s % 4

        @pl.when(s < 4)
        def _():
            load_leg(tt).wait()
            load_leg(tt + 4).wait()

        rows = lax.broadcasted_iota(jnp.int32, (256, 768), 0)
        lanes = lax.broadcasted_iota(jnp.int32, (256, 768), 1) % 16
        rh, mh = rows // 128, rows % 8
        swapped = (par == 1) & (mh > 0)
        mask = lanes == jnp.where(swapped, 8 - 8 * rh, 8 * rh) + mh
        values = arrived[g, :, tt].reshape(256, 128)
        lhs = []
        for h in range(2):
            ex = jnp.concatenate([
                lax.dot_general(values, expand[h, part], CONTRACT_ROWS, preferred_element_type=F32)
                for part in range(2)], axis=0)
            lhs.append(jnp.where(mask, ex, 0.0).astype(BF))
        for bx in range(4):
            pa, pb = [
                jnp.dot(lhs[h], leg[tt + 4 * h, :, :, 256 * bx:256 * bx + 256].reshape(768, 256),
                        preferred_element_type=F32)
                for h in range(2)
            ]
            for half in range(2):
                a = pa[:, 128 * half:128 * half + 128]
                b = pb[:, 128 * half:128 * half + 128]
                first = jnp.where(low_lanes, a, pltpu.roll(b, 64, 1))
                second = jnp.where(low_lanes, pltpu.roll(a, 64, 1), b)
                for bz, value in ((2 * half, first), (2 * half + 1, second)):
                    q[qs, bx * (1 - par) + bz * par, bz * (1 - par) + bx * par] = value
        i = x * (1 - par) + z * par
        c1, c2, c3 = (i + 1) % 4, (i + 2) % 4, (i + 3) % 4
        minus, plus = copies(s, 0, ms1, mr1, par)
        ms1[s, 0, 0] = q[qs, c2, :, A, :].astype(BF)
        ms1[s, 0, 1] = q[qs, c3, :, B, :].astype(BF)
        minus.start()
        ms1[s, 1, 0] = q[qs, c2, :, B, :].astype(BF)
        ms1[s, 1, 1] = q[qs, c1, :, A, :].astype(BF)
        plus.start()

    def relay1(s):
        par, qs = s % 2, s % 4
        i = x * (1 - par) + z * par
        c1, c3 = (i + 1) % 4, (i + 3) % 4
        minus, plus = copies(s, 0, ms1, mr1, par)
        send = copies(s, 1, ss1, sr1, par)
        minus.wait_recv()
        ss1[s, 0] = (q[qs, c3, :, A, :] + mr1[s, 0, 0].astype(F32)).astype(BF)
        send[0].start()
        plus.wait_recv()
        ss1[s, 1] = (q[qs, c1, :, B, :] + mr1[s, 1, 0].astype(F32)).astype(BF)
        send[1].start()

    def owner1(s):
        par, qs = s % 2, s % 4
        i = x * (1 - par) + z * par
        minus, plus = copies(s, 1, ss1, sr1, par)
        minus.wait_recv()
        q2[s, :, A, :] = q[qs, i, :, A, :] + mr1[s, 1, 1].astype(F32) + sr1[s, 0].astype(F32)
        plus.wait_recv()
        q2[s, :, B, :] = q[qs, i, :, B, :] + mr1[s, 0, 1].astype(F32) + sr1[s, 1].astype(F32)
        j = z * (1 - par) + x * par
        d1, d2, d3 = (j + 1) % 4, (j + 2) % 4, (j + 3) % 4
        ms2[s, 0, 0] = q2[s, d2, A, :].astype(BF)
        ms2[s, 0, 1] = q2[s, d3, B, :].astype(BF)
        ms2[s, 1, 0] = q2[s, d2, B, :].astype(BF)
        ms2[s, 1, 1] = q2[s, d1, A, :].astype(BF)
        for copy in copies(s, 2, ms2, mr2, 1 - par):
            copy.start()

    def relay2(s):
        par = s % 2
        j = z * (1 - par) + x * par
        d1, d3 = (j + 1) % 4, (j + 3) % 4
        minus, plus = copies(s, 2, ms2, mr2, 1 - par)
        send = copies(s, 3, ss2, sr2, 1 - par)
        minus.wait_recv()
        ss2[s, 0] = (q2[s, d3, A, :] + mr2[s, 0, 0].astype(F32)).astype(BF)
        send[0].start()
        plus.wait_recv()
        ss2[s, 1] = (q2[s, d1, B, :] + mr2[s, 1, 0].astype(F32)).astype(BF)
        send[1].start()

    def owner2(s):
        par = s % 2
        j = z * (1 - par) + x * par
        minus, plus = copies(s, 3, ss2, sr2, 1 - par)
        minus.wait_recv()
        final[s, A, :] = q2[s, j, A, :] + mr2[s, 1, 1].astype(F32) + sr2[s, 0].astype(F32)
        plus.wait_recv()
        final[s, B, :] = q2[s, j, B, :] + mr2[s, 0, 1].astype(F32) + sr2[s, 1].astype(F32)

    def output_group(g):
        top_row = lax.broadcasted_iota(jnp.int32, (8, 128), 0) == 0

        def column(fc, carry):
            pieces = []
            for tt in range(4):
                v0 = final[4 * g + tt, pl.ds(pl.multiple_of(8 * fc, 8), 8), :]
                v1 = final[4 * g + tt, pl.ds(pl.multiple_of(128 + 8 * fc, 8), 8), :]
                if tt % 2:
                    v0, v1 = jnp.where(top_row, v0, v1), jnp.where(top_row, v1, v0)
                pieces += [v0, v1]
            turned = jnp.concatenate(pieces, axis=0).T
            out_row = (fc // 2 * 2 + g) * 2 + fc % 2
            out_ref[pl.ds(out_row, 64, stride=32), :] = jnp.concatenate([turned[0:64], turned[64:128]], axis=1)
            return carry

        lax.fori_loop(0, 16, column, 0)

    stages = tuple(zip((compute, relay1, owner1, relay2, owner2), LAGS))
    last = FIRST + LAGS[-1] + 4

    def step(k, carry):
        @pl.when(k < 2)
        def _():
            pass_on(k)

        @pl.when((k == 0) | (k == STEP_A))
        def _():
            transform_group((k + STEP_A - 1) // STEP_A)

        @pl.when(k == 0)
        def _():
            for d, other in pairs:
                near(1, d, other).start()

        @pl.when((k == 1) | (k == STEP_B))
        def _():
            place_group((k + STEP_B - 2) // STEP_B)

        @pl.when((k == 2) | (k == STEP_C))
        def _():
            receive_group((k + STEP_C - 3) // STEP_C)

        for stage, lag in stages:
            start = FIRST + lag

            @pl.when(((k >= start) & (k < start + 4)) | ((k >= start + 4 + DELAY) & (k < start + 8 + DELAY)))
            def _():
                late = (k - start) // (4 + DELAY)
                stage(k - start - late * DELAY)

        @pl.when((k == last) | (k == last + 4 + DELAY))
        def _():
            output_group((k - last) // (4 + DELAY))

        return carry

    lax.fori_loop(0, last + 5 + DELAY, step, 0)

    def drain(s, carry):
        par = s % 2
        for kind, src, dst, axis in ((0, ms1, mr1, par), (1, ss1, sr1, par), (2, ms2, mr2, 1 - par), (3, ss2, sr2, 1 - par)):
            for copy in copies(s, kind, src, dst, axis):
                copy.wait_send()
        return carry

    lax.fori_loop(0, NBLOCK, drain, 0)

    def drain_group(g, carry):
        for d, other in pairs:
            far(g, d, other).wait_send()
            near(g, d, other).wait_send()
            forward(g, d, other).wait_send()
        side(g).wait_send()
        for dy, dc in order_peers:
            exchange_order(g, dy, dc).wait_send()
        for dx, dz in blk_peers:
            exchange_blk(g, dx, dz).wait_send()
        return carry

    lax.fori_loop(0, 2, drain_group, 0)


def analysis(field, mask, plan, legendre):
    high, low = dft_tables()
    vmem, anywhere = pl.BlockSpec(memory_space=pltpu.VMEM), pl.BlockSpec(memory_space=pl.ANY)
    dma = pltpu.SemaphoreType.DMA
    half = (NBLOCK, 2, 4, 128, 128)
    return pl.pallas_call(
        kernel,
        out_shape=jax.ShapeDtypeStruct((2048, 128), F32),
        in_specs=[anywhere, anywhere, vmem, anywhere, anywhere, anywhere, anywhere],
        out_specs=vmem,
        scratch_shapes=[
            pltpu.VMEM((16, 64, 512), F32),
            pltpu.VMEM((64, 512), jnp.int32),
            pltpu.VMEM((16, 128, 256), BF), pltpu.VMEM((16, 128, 256), BF), pltpu.VMEM((128, 128), BF),
            pltpu.VMEM((2, 8, 64, 512), F32),
            pltpu.VMEM((2, 2, 2, 32, 512), F32),
            pltpu.VMEM((16, 64, 512), BF),
            pltpu.VMEM((8, 8, 16, 128), BF),
            pltpu.VMEM((2, 8, 8, 16, 128), BF), pltpu.VMEM((2, 8, 8, 16, 128), BF),
            pltpu.VMEM((128, 128), BF), pltpu.VMEM((2, 2, 256, 768), BF),
            pltpu.VMEM((2, 16, 4, 16, 128), BF), pltpu.VMEM((2, 16, 4, 16, 128), BF),
            pltpu.VMEM((8, 48, 16, 1024), BF),
            pltpu.VMEM((4, 4, 4, 256, 128), F32),
            pltpu.VMEM((NBLOCK, 4, 256, 128), F32),
            pltpu.VMEM((NBLOCK, 2, 2, 4, 128, 128), BF), pltpu.VMEM((NBLOCK, 2, 2, 4, 128, 128), BF),
            pltpu.VMEM(half, BF), pltpu.VMEM(half, BF),
            pltpu.VMEM((NBLOCK, 2, 2, 128, 128), BF), pltpu.VMEM((NBLOCK, 2, 2, 128, 128), BF),
            pltpu.VMEM((NBLOCK, 2, 128, 128), BF), pltpu.VMEM((NBLOCK, 2, 128, 128), BF),
            pltpu.VMEM((NBLOCK, 256, 128), F32),
            dma((16,)), dma((4,)), dma((8,)),
            dma((2, 2, 2)), dma((2, 2, 2)), dma((2, 2, 2)), dma((2, 2, 2)), dma((2, 2, 2)), dma((2, 2, 2)),
            dma((2,)), dma((2,)), dma((2, 4, 2)), dma((2, 4, 2)), dma((2, 4, 4)), dma((2, 4, 4)),
            dma((NBLOCK, 4, 2)), dma((NBLOCK, 4, 2)),
        ],
        compiler_params=pltpu.CompilerParams(collective_id=0, has_side_effects=True, vmem_limit_bytes=62 * 2**20),
    )(field, mask, plan.reshape(16, 64), jnp.asarray(high), jnp.asarray(low), jnp.asarray(order_permutation()), legendre)


def body(field, ocean_mask, plan, legendre):
    return analysis(field, ocean_mask, plan, legendre).reshape(64, 16, 2, 128)


def solution(mesh):
    placed = (P(None, "blk", "order"), P("blk", "order"), P(), P("blk", "order", None))
    return jax.shard_map(
        body, mesh=mesh, in_specs=placed, out_specs=P("blk", None, None, "order"), check_vma=False
    )
```

```python
import math

import jax
import jax.numpy as jnp
import numpy as np
from jax import lax
from jax.experimental import pallas as pl
from jax.experimental.pallas import tpu as pltpu
from jax.sharding import PartitionSpec as P

NLON = 4096
MESH = pl.DeviceIdType.MESH
BF = jnp.bfloat16
F32 = jnp.float32
NBLOCK = 8
CONTRACT_LANES = (((1,), (1,)), ((), ()))
CONTRACT_ROWS = (((0,), (0,)), ((), ()))

PIECES = 2
SPAN = 4 // PIECES
SCHEDULE = (
    "P0", "F1", "M0", "A0", "N1", "P1", "B00", "B01", "C00", "m0", "m1", "C01", "m2", "A1", "m3", "r0", "r1", "B10",
    "B11", "r2", "o0", "r3", "o1", "C10", "m4", "C11", "m5", "o2", "o3", "m6", "m7", "R0", "R1", "r4", "r5", "R2",
    "R3", "r6", "r7", "o4", "o5", "O0", "O1", "O2", "O3", "T0", "R4", "o6", "R5", "o7", "D", "R6", "R7", "O4", "O5",
    "O6", "O7", "T1", "E",
)


def dft_tables():
    r = np.arange(16)[:, None, None]
    column = np.arange(64)[None, :, None]
    owner, w, ql = column // 8, column // 4 % 2, column % 4
    residue = np.where(w == 0, r, np.where(r == 0, 16, 32 - r))
    m = 32 * (4 * owner + ql) + residue
    i = np.arange(128)[None, None, :]
    angle = 2.0 * np.pi * (m * i % NLON) / NLON
    real, imag = np.cos(angle) / 64.0, np.where(w == 0, 1.0, -1.0) * np.sin(angle) / 64.0
    table = np.concatenate([real, imag], axis=2).astype(np.float32)
    high = table.astype(jnp.bfloat16)
    low = (table - high.astype(np.float32)).astype(jnp.bfloat16)
    return high, low


def order_permutation():
    out = np.zeros((128, 128), np.float32)
    for r in range(8):
        for w in range(2):
            for c in range(2):
                for ql in range(4):
                    mh = r if w == 0 else (8 - r) % 8
                    t = 2 * ql + w
                    out[(t % 4 * 2 + t // 4) * 16 + c * 8 + mh, r * 16 + c * 8 + w * 4 + ql] = 1.0
    return out.astype(jnp.bfloat16)


def real_dft(values):
    n = len(values)
    if n == 2:
        return [(values[0] + values[1], None), (values[0] - values[1], None)]
    even, odd = real_dft(values[0::2]), real_dft(values[1::2])
    half = n // 2

    def term(part, k):
        if k <= half // 2:
            return part[k]
        re, im = part[half - k]
        return re, (None if im is None else -im)

    result = [None] * (half + 1)
    for k in range(half // 2 + 1):
        er, ei = even[k]
        qr, qi = odd[k]
        cos, sin = math.cos(2 * math.pi * k / n), math.sin(2 * math.pi * k / n)
        if k == 0:
            result[0] = (er + qr, None)
            result[half] = (er - qr, None)
            continue
        if 4 * k == n:
            tr, ti = qi, -qr
        else:
            tr = qr * cos + qi * sin if qi is not None else qr * cos
            ti = qi * cos - qr * sin if qi is not None else -(qr * sin)

        def add(a, b, sign):
            if a is None:
                return None if b is None else (b if sign > 0 else -b)
            if b is None:
                return a
            return a + b if sign > 0 else a - b

        result[k] = (add(er, tr, 1), add(ei, ti, 1))
        if k != half - k:
            ni = add(ei, ti, -1)
            result[half - k] = (add(er, tr, -1), None if ni is None else -ni)
    return result


def kernel(field_hbm, mask_hbm, plan_ref, high_hbm, low_hbm, perm_hbm, leg_hbm, out_ref,
           masked, mask, table, perm, xr, relay, ycat, terms, sbuf, srecv, place, expand, sent, arrived,
           leg, q, q2, ms1, mr1, ss1, sr1, ms2, mr2, ss2, sr2, final,
           field_sem, load_sem, leg_sem, far_s, far_r, near_s, near_r, fwd_s, fwd_r, side_s, side_r,
           ox_s, ox_r, bx_s, bx_r, ring_s, ring_r):
    order = lax.axis_index("order")
    y, core = order // 2, order % 2
    me = lax.axis_index("blk")
    x, z = me // 4, me % 4

    def load_field(g, o):
        f = 2 * o + g
        return pltpu.make_async_copy(field_hbm.at[f], masked.at[f], field_sem.at[g])

    loads = [pltpu.make_async_copy(src, dst, load_sem.at[i]) for i, (src, dst) in enumerate(
        ((mask_hbm, mask), (high_hbm, table.at[:, pl.ds(0, 64), 0:256]),
         (low_hbm, table.at[:, pl.ds(0, 64), 512:768]), (perm_hbm, perm)))]

    def load_leg(t):
        return pltpu.make_async_copy(leg_hbm.at[:, pl.ds(16 * t, 16), :], leg.at[t // 4, t % 4], leg_sem.at[t % 4])

    loads[0].start()
    for o in range(8):
        load_field(0, o).start()

    barrier = pltpu.get_barrier_semaphore()
    order_peers = [(dy, dc) for dy in range(4) for dc in range(2) if (dy, dc) != (0, 0)]
    blk_peers = [(dx, dz) for dx in range(4) for dz in range(4) if (dx, dz) != (0, 0)]

    def at(dy, other):
        return {"order": (y + dy) % 4 * 2 + other}

    for dy, dc in order_peers:
        pl.semaphore_signal(barrier, inc=1, device_id=at(dy, (core + dc) % 2), device_id_type=MESH)
    for dx, dz in blk_peers:
        pl.semaphore_signal(barrier, inc=1, device_id={"blk": (x + dx) % 4 * 4 + (z + dz) % 4}, device_id_type=MESH)

    for o in range(8):
        load_field(1, o).start()
    for copy in loads[1:]:
        copy.start()
    loads[0].wait()

    def mask_fields(g):
        pltpu.make_async_copy(field_hbm.at[pl.ds(0, 8)], masked.at[pl.ds(0, 8)], field_sem.at[g]).wait()

        def one(o, carry):
            masked[2 * o + g] = masked[2 * o + g] * mask[...].astype(F32)
            return carry

        lax.fori_loop(0, 8, one, 0)
        xr[g, order] = masked[order * 2 + g]

    def remote(src, dst, ss, rs, device):
        return pltpu.make_async_remote_copy(src_ref=src, dst_ref=dst, send_sem=ss, recv_sem=rs,
                                            device_id=device, device_id_type=MESH)

    halves = (pl.ds(0, 32), pl.ds(32, 32))
    steps = (1, 3)
    pairs = [(d, other) for d in range(2) for other in range(2)]

    def far(g, d, other):
        target = ((y + 2) % 4 * 2 + other) * 2 + g
        return remote(masked.at[target, halves[d]], relay.at[g, d, core], far_s.at[g], far_r.at[g, d, core],
                      at(steps[d], other))

    def near(g, d, other):
        target = ((y + steps[d]) % 4 * 2 + other) * 2 + g
        return remote(masked.at[target], xr.at[g, order], near_s.at[g], near_r.at[g],
                      at(steps[d], other))

    def forward(g, d, source):
        origin = (y + 4 - steps[d]) % 4 * 2 + source
        return remote(relay.at[g, d, source], xr.at[g, origin, halves[d]], fwd_s.at[g], fwd_r.at[g],
                      at(steps[d], core))

    def side(g):
        target = (y * 2 + 1 - core) * 2 + g
        return remote(masked.at[target], xr.at[g, order], side_s.at[g], side_r.at[g], at(0, 1 - core))

    def wait_far(g, d, source):
        remote(masked.at[0, halves[d]], relay.at[g, d, source], far_s.at[g], far_r.at[g, d, source],
               at(steps[d], source)).wait_recv()

    def all_far(g):
        return remote(relay.at[g], relay.at[g], far_s.at[g], far_r.at[g, 0, 0], at(1, 0))

    def all_near(g):
        part = pl.ds(0, 4)
        return remote(xr.at[g, part], xr.at[g, part], near_s.at[g], near_r.at[g], at(1, 0))

    def all_forward(g):
        return remote(relay.at[g], relay.at[g], fwd_s.at[g], fwd_r.at[g], at(1, 0))

    mask_fields(0)
    pl.semaphore_wait(barrier, 22)
    for d, other in pairs:
        far(0, d, other).start()
    for d, other in pairs:
        near(0, d, other).start()
    side(0).start()
    for t in range(8):
        load_leg(t).start()
    mask_fields(1)
    side(1).start()

    earlier = (lax.broadcasted_iota(jnp.int32, (64, 64), 0) < lax.broadcasted_iota(jnp.int32, (64, 64), 1))
    earlier = earlier.astype(F32).astype(BF)

    def owner_of(b, rows):
        both = plan_ref[pl.ds(b // 2, 1), :]
        slots = jnp.broadcast_to(jnp.where(b % 2 == 0, both[:, 0:64], both[:, 64:128]), (rows, 64))
        owner = jnp.zeros((rows, 64), jnp.int32)
        for b in range(1, 17):
            owner += (slots >= 48 * b).astype(jnp.int32)
        return slots, owner

    def source_maps(_):
        row = lax.broadcasted_iota(jnp.int32, (128, 64), 0)
        _, owner = owner_of(me, 128)
        mine = owner == row // 8
        count = jnp.dot(mine.astype(F32).astype(BF), earlier, preferred_element_type=F32)
        match = mine & (count == (row // 2 % 4).astype(F32))
        for rh in range(2):
            place[:, 64 * rh:64 * rh + 64] = (match & (row % 2 == rh)).astype(F32).astype(BF)

        def source_map(b, carry):
            slots, owner = owner_of(b, 16)
            mine = owner == me
            count = jnp.dot(mine.astype(F32).astype(BF), earlier, preferred_element_type=F32)
            rows = lax.broadcasted_iota(jnp.int32, (16, 64), 0)
            match = mine & (count == (rows // 2 % 4).astype(F32))
            slot = jnp.sum(jnp.where(match, (slots - 48 * me + 1).astype(F32), 0.0), axis=1, keepdims=True)
            lanes = lax.broadcasted_iota(jnp.int32, (16, 768), 1) // 16 + 1
            rows = lax.broadcasted_iota(jnp.int32, (16, 768), 0)
            hit = jnp.broadcast_to(slot, (16, 768)) == lanes.astype(F32)
            for h in range(2):
                for rh in range(2):
                    expand[h, rh, pl.ds(pl.multiple_of(16 * b, 16), 16), :] = (
                        hit & (rows // 8 == h) & (rows % 2 == rh)).astype(F32).astype(BF)
            return carry

        lax.fori_loop(0, 16, source_map, 0)
        for copy in loads[1:]:
            copy.wait()

        w = lax.broadcasted_iota(jnp.int32, (64, 128), 0) // 4 % 2

        def complete(r, carry):
            for start in (0, 512):
                real = table[r, 0:64, start:start + 128].astype(F32)
                imag = table[r, 0:64, start + 128:start + 256].astype(F32)
                sign = jnp.where(w == 0, 1.0, -1.0)
                special = jnp.broadcast_to(r == 0, (64, 128))
                parts = (
                    (jnp.where(special & (w == 1), 0.0, real), jnp.where(special, jnp.where(w == 1, real, 0.0), imag)),
                    (jnp.where(special & (w == 1), 0.0, -sign * imag),
                     jnp.where(special, jnp.where(w == 1, imag, 0.0), sign * real)),
                )
                for c in range(2):
                    for half in range(2):
                        value = parts[c][half].astype(BF)
                        table[r, 64 * c:64 * c + 64, start + 128 * half:start + 128 * half + 128] = value
                        if start == 0:
                            table[r, 64 * c:64 * c + 64, 256 + 128 * half:384 + 128 * half] = value
            return carry

        lax.fori_loop(0, 16, complete, 0)

    def exchange_order(g, piece, peer):
        target = (y + peer // 2) % 4 * 2 + (core + peer) % 2
        rows = pl.ds(2 * SPAN * piece, 2 * SPAN)
        return remote(sbuf.at[g, target, rows], srecv.at[g, order, rows], ox_s.at[g, piece], ox_r.at[g, piece],
                      {"order": target})

    def exchange_blk(g, piece, peer):
        target = (x + peer // 4) % 4 * 4 + (z + peer) % 4
        rows = pl.ds(SPAN * piece, SPAN)
        return remote(sent.at[g, target, rows], arrived.at[g, me, rows], bx_s.at[g, piece], bx_r.at[g, piece],
                      {"blk": target})

    def all_order(g, piece):
        part = srecv.at[g, pl.ds(0, 7), pl.ds(2 * SPAN * piece, 2 * SPAN)]
        return remote(part, part, ox_s.at[g, piece], ox_r.at[g, piece], at(1, 0))

    def all_blk(g, piece):
        part = arrived.at[g, pl.ds(0, 15), pl.ds(SPAN * piece, SPAN)]
        return remote(part, part, bx_s.at[g, piece], bx_r.at[g, piece], {"blk": (me + 1) % 16})

    order_first = (4, 5, 2, 3, 6, 7, 1)
    blk_first = (10, 9, 11, 6, 14, 8, 2, 5, 7, 13, 15, 1, 3, 4, 12)

    def pass_on(g):
        for d, source in pairs:
            wait_far(g, d, source)
            forward(g, d, source).start()

    def transform_group(g):
        all_near(g).wait_recv()
        side(g).wait_recv()
        all_forward(g).wait_recv()

        def butterfly(k, carry):
            rows = pl.ds(pl.multiple_of(16 * k, 16), 16)
            values = [xr[g, a // 4, rows, 128 * (a % 4):128 * (a % 4) + 128] for a in range(32)]
            result = real_dft(values)
            for r in range(16):
                pair = (result[0][0], result[16][0]) if r == 0 else result[r]
                for part, value in enumerate(pair):
                    top = value.astype(BF)
                    ycat[r, rows, 128 * part:128 * part + 128] = top
                    ycat[r, rows, 256 + 128 * part:384 + 128 * part] = (value - top.astype(F32)).astype(BF)
                    ycat[r, rows, 512 + 128 * part:640 + 128 * part] = top
            return carry

        lax.fori_loop(0, 4, butterfly, 0)

        for r in range(8):
            parts = [lax.dot_general(table[rr], ycat[rr], CONTRACT_LANES, preferred_element_type=F32) for rr in (r, r + 8)]
            both = jnp.concatenate(parts, axis=1)
            for o in range(8):
                rows = jnp.concatenate([both[8 * o:8 * o + 8], both[64 + 8 * o:64 + 8 * o + 8]], axis=0)
                terms[16 * r:16 * r + 16, 128 * o:128 * o + 128] = rows.astype(BF)
        part = jnp.dot(perm[...], terms[...], preferred_element_type=F32).astype(BF)
        for o in range(8):
            sbuf[g, o] = part[:, 128 * o:128 * o + 128].reshape(8, 16, 128)
        for piece in range(PIECES):
            for peer in order_first:
                exchange_order(g, piece, peer).start()
        srecv[g, order] = sbuf[g, order]

    def place_group(g, piece):
        all_order(g, piece).wait_recv()
        for tt in range(SPAN * piece, SPAN * piece + SPAN):
            parts = []
            for h in range(2):
                rows = srecv[g, :, 2 * tt + h].reshape(128, 128)
                out = lax.dot_general(place[...], rows, CONTRACT_LANES, preferred_element_type=F32)
                parts.append(out.reshape(16, 8, 128))
            sent[g, :, tt] = jnp.concatenate(parts, axis=1).astype(BF)
            arrived[g, me, tt] = sent[g, me, tt]
        for peer in blk_first:
            exchange_blk(g, piece, peer).start()

    def receive_group(g, piece):
        all_blk(g, piece).wait_recv()

    low_lanes = lax.broadcasted_iota(jnp.int32, (256, 128), 1) < 64

    def neighbour(axis, step):
        nx = (x + step * (1 - axis)) % 4
        nz = (z + step * axis) % 4
        return {"blk": nx * 4 + nz}

    def copies(s, kind, src, dst, axis):
        return [remote(src.at[s, way], dst.at[s, way], ring_s.at[s, kind], ring_r.at[s, kind],
                       neighbour(axis, 3 - 2 * way)) for way in range(2)]

    def ring(s, kind, src, dst):
        return remote(src.at[s], dst.at[s], ring_s.at[s, kind], ring_r.at[s, kind], {"blk": (me + 1) % 16})

    A, B = pl.ds(0, 128), pl.ds(128, 128)

    def compute(s):
        g, tt, par, qs = s // 4, s % 4, s % 2, s % 4

        if s < 4:
            pltpu.make_async_copy(leg.at[:, tt], leg.at[:, tt], leg_sem.at[tt]).wait()

        rows = lax.broadcasted_iota(jnp.int32, (256, 768), 0)
        lanes = lax.broadcasted_iota(jnp.int32, (256, 768), 1) % 16
        rh, mh = rows // 128, rows % 8
        swapped = (par == 1) & (mh > 0)
        mask = lanes == jnp.where(swapped, 8 - 8 * rh, 8 * rh) + mh
        values = arrived[g, :, tt].reshape(256, 128)
        lhs = []
        for h in range(2):
            ex = jnp.concatenate([
                lax.dot_general(values, expand[h, part], CONTRACT_ROWS, preferred_element_type=F32)
                for part in range(2)], axis=0)
            lhs.append(jnp.where(mask, ex, 0.0).astype(BF))
        for bx in range(4):
            pa, pb = [
                jnp.dot(lhs[h], leg[h, tt, :, :, 256 * bx:256 * bx + 256].reshape(768, 256),
                        preferred_element_type=F32)
                for h in range(2)
            ]
            for half in range(2):
                a = pa[:, 128 * half:128 * half + 128]
                b = pb[:, 128 * half:128 * half + 128]
                first = jnp.where(low_lanes, a, pltpu.roll(b, 64, 1))
                second = jnp.where(low_lanes, pltpu.roll(a, 64, 1), b)
                for bz, value in ((2 * half, first), (2 * half + 1, second)):
                    q[qs, bx * (1 - par) + bz * par, bz * (1 - par) + bx * par] = value
        i = x * (1 - par) + z * par
        c1, c2, c3 = (i + 1) % 4, (i + 2) % 4, (i + 3) % 4
        minus, plus = copies(s, 0, ms1, mr1, par)
        ms1[s, 0, 0] = q[qs, c2, :, A, :].astype(BF)
        ms1[s, 0, 1] = q[qs, c3, :, B, :].astype(BF)
        minus.start()
        ms1[s, 1, 0] = q[qs, c2, :, B, :].astype(BF)
        ms1[s, 1, 1] = q[qs, c1, :, A, :].astype(BF)
        plus.start()

    def relay1(s):
        par, qs = s % 2, s % 4
        i = x * (1 - par) + z * par
        c1, c3 = (i + 1) % 4, (i + 3) % 4
        send = copies(s, 1, ss1, sr1, par)
        ring(s, 0, ms1, mr1).wait_recv()
        ss1[s, 0] = (q[qs, c3, :, A, :] + mr1[s, 0, 0].astype(F32)).astype(BF)
        send[0].start()
        ss1[s, 1] = (q[qs, c1, :, B, :] + mr1[s, 1, 0].astype(F32)).astype(BF)
        send[1].start()

    def owner1(s):
        par, qs = s % 2, s % 4
        i = x * (1 - par) + z * par
        ring(s, 1, ss1, sr1).wait_recv()
        q2[s, :, A, :] = q[qs, i, :, A, :] + mr1[s, 1, 1].astype(F32) + sr1[s, 0].astype(F32)
        q2[s, :, B, :] = q[qs, i, :, B, :] + mr1[s, 0, 1].astype(F32) + sr1[s, 1].astype(F32)
        j = z * (1 - par) + x * par
        d1, d2, d3 = (j + 1) % 4, (j + 2) % 4, (j + 3) % 4
        ms2[s, 0, 0] = q2[s, d2, A, :].astype(BF)
        ms2[s, 0, 1] = q2[s, d3, B, :].astype(BF)
        ms2[s, 1, 0] = q2[s, d2, B, :].astype(BF)
        ms2[s, 1, 1] = q2[s, d1, A, :].astype(BF)
        for copy in copies(s, 2, ms2, mr2, 1 - par):
            copy.start()

    def relay2(s):
        par = s % 2
        j = z * (1 - par) + x * par
        d1, d3 = (j + 1) % 4, (j + 3) % 4
        send = copies(s, 3, ss2, sr2, 1 - par)
        ring(s, 2, ms2, mr2).wait_recv()
        ss2[s, 0] = (q2[s, d3, A, :] + mr2[s, 0, 0].astype(F32)).astype(BF)
        send[0].start()
        ss2[s, 1] = (q2[s, d1, B, :] + mr2[s, 1, 0].astype(F32)).astype(BF)
        send[1].start()

    def owner2(s):
        par = s % 2
        j = z * (1 - par) + x * par
        ring(s, 3, ss2, sr2).wait_recv()
        final[s, A, :] = q2[s, j, A, :] + mr2[s, 1, 1].astype(F32) + sr2[s, 0].astype(F32)
        final[s, B, :] = q2[s, j, B, :] + mr2[s, 0, 1].astype(F32) + sr2[s, 1].astype(F32)

    def output_group(g):
        top_row = lax.broadcasted_iota(jnp.int32, (8, 128), 0) == 0

        def column(fc, carry):
            pieces = []
            for tt in range(4):
                v0 = final[4 * g + tt, pl.ds(pl.multiple_of(8 * fc, 8), 8), :]
                v1 = final[4 * g + tt, pl.ds(pl.multiple_of(128 + 8 * fc, 8), 8), :]
                if tt % 2:
                    v0, v1 = jnp.where(top_row, v0, v1), jnp.where(top_row, v1, v0)
                pieces += [v0, v1]
            turned = jnp.concatenate(pieces, axis=0).T
            out_row = (fc // 2 * 2 + g) * 2 + fc % 2
            out_ref[pl.ds(out_row, 64, stride=32), :] = jnp.concatenate([turned[0:64], turned[64:128]], axis=1)
            return carry

        lax.fori_loop(0, 16, column, 0, unroll=4)

    def near_group(g):
        for d, other in pairs:
            near(g, d, other).start()

    def far_group(g):
        for d, other in pairs:
            far(g, d, other).start()

    def ring_drain(s, kinds):
        for kind in kinds:
            src, dst = ((ms1, mr1), (ss1, sr1), (ms2, mr2), (ss2, sr2))[kind]
            ring(s, kind, src, dst).wait_send()

    def drain_early():
        for g in range(2):
            all_far(g).wait_send()
            all_near(g).wait_send()
            all_forward(g).wait_send()
            side(g).wait_send()
            for piece in range(PIECES):
                all_order(g, piece).wait_send()
                all_blk(g, piece).wait_send()
        for s in range(4):
            ring_drain(s, (0, 1, 2, 3))
        for s in range(4, 8):
            ring_drain(s, (0,))

    def drain_late():
        for s in range(4, 8):
            ring_drain(s, (1, 2, 3))

    run = dict(F=far_group, N=near_group, P=pass_on, A=transform_group, B=place_group, C=receive_group, M=source_maps,
               m=compute, r=relay1, o=owner1, R=relay2, O=owner2, T=output_group, D=drain_early, E=drain_late)
    for name in SCHEDULE:
        run[name[0]](*map(int, name[1:]))


def analysis(field, mask, plan, legendre):
    high, low = dft_tables()
    vmem, anywhere = pl.BlockSpec(memory_space=pltpu.VMEM), pl.BlockSpec(memory_space=pl.ANY)
    dma = pltpu.SemaphoreType.DMA
    half = (NBLOCK, 2, 4, 128, 128)
    return pl.pallas_call(
        kernel,
        out_shape=jax.ShapeDtypeStruct((2048, 128), F32),
        in_specs=[anywhere, anywhere, vmem, anywhere, anywhere, anywhere, anywhere],
        out_specs=vmem,
        scratch_shapes=[
            pltpu.VMEM((16, 64, 512), F32),
            pltpu.VMEM((64, 512), jnp.int32),
            pltpu.VMEM((16, 128, 768), BF), pltpu.VMEM((128, 128), BF),
            pltpu.VMEM((2, 8, 64, 512), F32),
            pltpu.VMEM((2, 2, 2, 32, 512), F32),
            pltpu.VMEM((16, 64, 768), BF),
            pltpu.VMEM((128, 1024), BF),
            pltpu.VMEM((2, 8, 8, 16, 128), BF), pltpu.VMEM((2, 8, 8, 16, 128), BF),
            pltpu.VMEM((128, 128), BF), pltpu.VMEM((2, 2, 256, 768), BF),
            pltpu.VMEM((2, 16, 4, 16, 128), BF), pltpu.VMEM((2, 16, 4, 16, 128), BF),
            pltpu.VMEM((2, 4, 48, 16, 1024), BF),
            pltpu.VMEM((4, 4, 4, 256, 128), F32),
            pltpu.VMEM((NBLOCK, 4, 256, 128), F32),
            pltpu.VMEM((NBLOCK, 2, 2, 4, 128, 128), BF), pltpu.VMEM((NBLOCK, 2, 2, 4, 128, 128), BF),
            pltpu.VMEM(half, BF), pltpu.VMEM(half, BF),
            pltpu.VMEM((NBLOCK, 2, 2, 128, 128), BF), pltpu.VMEM((NBLOCK, 2, 2, 128, 128), BF),
            pltpu.VMEM((NBLOCK, 2, 128, 128), BF), pltpu.VMEM((NBLOCK, 2, 128, 128), BF),
            pltpu.VMEM((NBLOCK, 256, 128), F32),
            dma((2,)), dma((4,)), dma((4,)),
            dma((2,)), dma((2, 2, 2)), dma((2,)), dma((2,)), dma((2,)), dma((2,)), dma((2,)), dma((2,)),
            dma((2, PIECES)), dma((2, PIECES)), dma((2, PIECES)), dma((2, PIECES)),
            dma((NBLOCK, 4)), dma((NBLOCK, 4)),
        ],
        compiler_params=pltpu.CompilerParams(collective_id=0, has_side_effects=True, vmem_limit_bytes=62 * 2**20),
    )(field, mask, plan.reshape(8, 128), jnp.asarray(high), jnp.asarray(low), jnp.asarray(order_permutation()), legendre)


def body(field, ocean_mask, plan, legendre):
    return analysis(field, ocean_mask, plan, legendre).reshape(64, 16, 2, 128)


def solution(mesh):
    placed = (P(None, "blk", "order"), P("blk", "order"), P(), P("blk", "order", None))
    return jax.shard_map(
        body, mesh=mesh, in_specs=placed, out_specs=P("blk", None, None, "order"), check_vma=False
    )
```

```python
import math

import jax
import jax.numpy as jnp
import numpy as np
from jax import lax
from jax.experimental import pallas as pl
from jax.experimental.pallas import tpu as pltpu
from jax.sharding import PartitionSpec as P

NLON = 4096
MESH = pl.DeviceIdType.MESH
BF = jnp.bfloat16
F32 = jnp.float32
NBLOCK = 8
CONTRACT_LANES = (((1,), (1,)), ((), ()))
CONTRACT_ROWS = (((0,), (0,)), ((), ()))

PIECES = 2
SPAN = 4 // PIECES
SCHEDULE = (
    "P0", "F1", "M0", "A0", "N1", "P1", "B00", "B01", "C00", "m0", "m1", "C01", "A1", "m2", "m3", "r0", "B10", "B11",
    "r1", "r2", "o0", "r3", "o1", "C10", "m4", "C11", "m5", "o2", "m6", "o3", "m7", "R0", "R1", "r4", "r5", "R2",
    "R3", "r6", "r7", "o4", "o5", "O0", "O1", "O2", "O3", "T0", "o6", "o7", "R4", "R5", "D", "R6", "R7", "O4", "O5",
    "O6", "O7", "T1", "E",
)


def dft_tables():
    r = np.arange(16)[:, None, None]
    column = np.arange(64)[None, :, None]
    owner, w, ql = column // 8, column // 4 % 2, column % 4
    residue = np.where(w == 0, r, np.where(r == 0, 16, 32 - r))
    m = 32 * (4 * owner + ql) + residue
    i = np.arange(128)[None, None, :]
    angle = 2.0 * np.pi * (m * i % NLON) / NLON
    real, imag = np.cos(angle) / 64.0, np.where(w == 0, 1.0, -1.0) * np.sin(angle) / 64.0
    table = np.concatenate([real, imag], axis=2).astype(np.float32)
    high = table.astype(jnp.bfloat16)
    low = (table - high.astype(np.float32)).astype(jnp.bfloat16)
    return high, low


def order_permutation():
    out = np.zeros((128, 128), np.float32)
    for r in range(8):
        for w in range(2):
            for c in range(2):
                for ql in range(4):
                    mh = r if w == 0 else (8 - r) % 8
                    t = 2 * ql + w
                    out[(t % 4 * 2 + t // 4) * 16 + c * 8 + mh, r * 16 + c * 8 + w * 4 + ql] = 1.0
    return out.astype(jnp.bfloat16)


def real_dft(values):
    n = len(values)
    if n == 2:
        return [(values[0] + values[1], None), (values[0] - values[1], None)]
    even, odd = real_dft(values[0::2]), real_dft(values[1::2])
    half = n // 2

    def term(part, k):
        if k <= half // 2:
            return part[k]
        re, im = part[half - k]
        return re, (None if im is None else -im)

    result = [None] * (half + 1)
    for k in range(half // 2 + 1):
        er, ei = even[k]
        qr, qi = odd[k]
        cos, sin = math.cos(2 * math.pi * k / n), math.sin(2 * math.pi * k / n)
        if k == 0:
            result[0] = (er + qr, None)
            result[half] = (er - qr, None)
            continue
        if 4 * k == n:
            tr, ti = qi, -qr
        else:
            tr = qr * cos + qi * sin if qi is not None else qr * cos
            ti = qi * cos - qr * sin if qi is not None else -(qr * sin)

        def add(a, b, sign):
            if a is None:
                return None if b is None else (b if sign > 0 else -b)
            if b is None:
                return a
            return a + b if sign > 0 else a - b

        result[k] = (add(er, tr, 1), add(ei, ti, 1))
        if k != half - k:
            ni = add(ei, ti, -1)
            result[half - k] = (add(er, tr, -1), None if ni is None else -ni)
    return result


def kernel(field_hbm, mask_hbm, plan_ref, high_hbm, low_hbm, perm_hbm, leg_hbm, out_ref,
           masked, mask, table, perm, xr, relay, ycat, terms, sbuf, srecv, place, expand, sent, arrived,
           leg, q, q2, ms1, mr1, ss1, sr1, ms2, mr2, ss2, sr2, final,
           field_sem, load_sem, leg_sem, far_s, far_r, near_s, near_r, fwd_s, fwd_r, side_s, side_r,
           ox_s, ox_r, bx_s, bx_r, ring_s, ring_r):
    order = lax.axis_index("order")
    y, core = order // 2, order % 2
    me = lax.axis_index("blk")
    x, z = me // 4, me % 4

    def load_field(g, o):
        f = 2 * o + g
        return pltpu.make_async_copy(field_hbm.at[f], masked.at[f], field_sem.at[g])

    loads = [pltpu.make_async_copy(src, dst, load_sem.at[i]) for i, (src, dst) in enumerate(
        ((mask_hbm, mask), (high_hbm, table.at[:, pl.ds(0, 64), 0:256]),
         (low_hbm, table.at[:, pl.ds(0, 64), 512:768]), (perm_hbm, perm)))]

    def load_leg(t):
        return pltpu.make_async_copy(leg_hbm.at[:, pl.ds(16 * t, 16), :], leg.at[t // 4, t % 4], leg_sem.at[t % 4])

    loads[0].start()
    for o in range(8):
        load_field(0, o).start()

    barrier = pltpu.get_barrier_semaphore()
    order_peers = [(dy, dc) for dy in range(4) for dc in range(2) if (dy, dc) != (0, 0)]
    blk_peers = [(dx, dz) for dx in range(4) for dz in range(4) if (dx, dz) != (0, 0)]

    def at(dy, other):
        return {"order": (y + dy) % 4 * 2 + other}

    for dy, dc in order_peers:
        pl.semaphore_signal(barrier, inc=1, device_id=at(dy, (core + dc) % 2), device_id_type=MESH)
    for dx, dz in blk_peers:
        pl.semaphore_signal(barrier, inc=1, device_id={"blk": (x + dx) % 4 * 4 + (z + dz) % 4}, device_id_type=MESH)

    for o in range(8):
        load_field(1, o).start()
    for copy in loads[1:]:
        copy.start()
    loads[0].wait()

    def mask_fields(g):
        pltpu.make_async_copy(field_hbm.at[pl.ds(0, 8)], masked.at[pl.ds(0, 8)], field_sem.at[g]).wait()

        def one(o, carry):
            masked[2 * o + g] = masked[2 * o + g] * mask[...].astype(F32)
            return carry

        lax.fori_loop(0, 8, one, 0)
        xr[g, order] = masked[order * 2 + g]

    def remote(src, dst, ss, rs, device):
        return pltpu.make_async_remote_copy(src_ref=src, dst_ref=dst, send_sem=ss, recv_sem=rs,
                                            device_id=device, device_id_type=MESH)

    halves = (pl.ds(0, 32), pl.ds(32, 32))
    steps = (1, 3)
    pairs = [(d, other) for d in range(2) for other in range(2)]

    def far(g, d, other):
        target = ((y + 2) % 4 * 2 + other) * 2 + g
        return remote(masked.at[target, halves[d]], relay.at[g, d, core], far_s.at[g], far_r.at[g, d, core],
                      at(steps[d], other))

    def near(g, d, other):
        target = ((y + steps[d]) % 4 * 2 + other) * 2 + g
        return remote(masked.at[target], xr.at[g, order], near_s.at[g], near_r.at[g],
                      at(steps[d], other))

    def forward(g, d, source):
        origin = (y + 4 - steps[d]) % 4 * 2 + source
        return remote(relay.at[g, d, source], xr.at[g, origin, halves[d]], fwd_s.at[g], fwd_r.at[g],
                      at(steps[d], core))

    def side(g):
        target = (y * 2 + 1 - core) * 2 + g
        return remote(masked.at[target], xr.at[g, order], side_s.at[g], side_r.at[g], at(0, 1 - core))

    def wait_far(g, d, source):
        remote(masked.at[0, halves[d]], relay.at[g, d, source], far_s.at[g], far_r.at[g, d, source],
               at(steps[d], source)).wait_recv()

    def all_far(g):
        return remote(relay.at[g], relay.at[g], far_s.at[g], far_r.at[g, 0, 0], at(1, 0))

    def all_near(g):
        part = pl.ds(0, 4)
        return remote(xr.at[g, part], xr.at[g, part], near_s.at[g], near_r.at[g], at(1, 0))

    def all_forward(g):
        return remote(relay.at[g], relay.at[g], fwd_s.at[g], fwd_r.at[g], at(1, 0))

    mask_fields(0)
    pl.semaphore_wait(barrier, 22)
    for d, other in pairs:
        far(0, d, other).start()
    for d, other in pairs:
        near(0, d, other).start()
    side(0).start()
    for t in range(8):
        load_leg(t).start()
    mask_fields(1)
    side(1).start()

    earlier = (lax.broadcasted_iota(jnp.int32, (64, 64), 0) < lax.broadcasted_iota(jnp.int32, (64, 64), 1))
    earlier = earlier.astype(F32).astype(BF)

    def owner_of(b, rows):
        both = plan_ref[pl.ds(b // 2, 1), :]
        slots = jnp.broadcast_to(jnp.where(b % 2 == 0, both[:, 0:64], both[:, 64:128]), (rows, 64))
        owner = jnp.zeros((rows, 64), jnp.int32)
        for b in range(1, 17):
            owner += (slots >= 48 * b).astype(jnp.int32)
        return slots, owner

    def source_maps(_):
        row = lax.broadcasted_iota(jnp.int32, (128, 64), 0)
        _, owner = owner_of(me, 128)
        mine = owner == row // 8
        count = jnp.dot(mine.astype(F32).astype(BF), earlier, preferred_element_type=F32)
        match = mine & (count == (row // 2 % 4).astype(F32))
        for rh in range(2):
            place[:, 64 * rh:64 * rh + 64] = (match & (row % 2 == rh)).astype(F32).astype(BF)

        def source_map(b, carry):
            slots, owner = owner_of(b, 16)
            mine = owner == me
            count = jnp.dot(mine.astype(F32).astype(BF), earlier, preferred_element_type=F32)
            rows = lax.broadcasted_iota(jnp.int32, (16, 64), 0)
            match = mine & (count == (rows // 2 % 4).astype(F32))
            slot = jnp.sum(jnp.where(match, (slots - 48 * me + 1).astype(F32), 0.0), axis=1, keepdims=True)
            lanes = lax.broadcasted_iota(jnp.int32, (16, 768), 1) // 16 + 1
            rows = lax.broadcasted_iota(jnp.int32, (16, 768), 0)
            hit = jnp.broadcast_to(slot, (16, 768)) == lanes.astype(F32)
            for h in range(2):
                for rh in range(2):
                    expand[h, rh, pl.ds(pl.multiple_of(16 * b, 16), 16), :] = (
                        hit & (rows // 8 == h) & (rows % 2 == rh)).astype(F32).astype(BF)
            return carry

        lax.fori_loop(0, 16, source_map, 0)
        for copy in loads[1:]:
            copy.wait()

        w = lax.broadcasted_iota(jnp.int32, (64, 128), 0) // 4 % 2

        def complete(r, carry):
            for start in (0, 512):
                real = table[r, 0:64, start:start + 128].astype(F32)
                imag = table[r, 0:64, start + 128:start + 256].astype(F32)
                sign = jnp.where(w == 0, 1.0, -1.0)
                special = jnp.broadcast_to(r == 0, (64, 128))
                parts = (
                    (jnp.where(special & (w == 1), 0.0, real), jnp.where(special, jnp.where(w == 1, real, 0.0), imag)),
                    (jnp.where(special & (w == 1), 0.0, -sign * imag),
                     jnp.where(special, jnp.where(w == 1, imag, 0.0), sign * real)),
                )
                for c in range(2):
                    for half in range(2):
                        value = parts[c][half].astype(BF)
                        table[r, 64 * c:64 * c + 64, start + 128 * half:start + 128 * half + 128] = value
                        if start == 0:
                            table[r, 64 * c:64 * c + 64, 256 + 128 * half:384 + 128 * half] = value
            return carry

        lax.fori_loop(0, 16, complete, 0)

    def exchange_order(g, piece, peer):
        target = (y + peer // 2) % 4 * 2 + (core + peer) % 2
        rows = pl.ds(2 * SPAN * piece, 2 * SPAN)
        return remote(sbuf.at[g, target, rows], srecv.at[g, order, rows], ox_s.at[g, piece], ox_r.at[g, piece],
                      {"order": target})

    def exchange_blk(g, piece, peer):
        target = (x + peer // 4) % 4 * 4 + (z + peer) % 4
        rows = pl.ds(SPAN * piece, SPAN)
        return remote(sent.at[g, target, rows], arrived.at[g, me, rows], bx_s.at[g, piece], bx_r.at[g, piece],
                      {"blk": target})

    def all_order(g, piece):
        part = srecv.at[g, pl.ds(0, 7), pl.ds(2 * SPAN * piece, 2 * SPAN)]
        return remote(part, part, ox_s.at[g, piece], ox_r.at[g, piece], at(1, 0))

    def all_blk(g, piece):
        part = arrived.at[g, pl.ds(0, 15), pl.ds(SPAN * piece, SPAN)]
        return remote(part, part, bx_s.at[g, piece], bx_r.at[g, piece], {"blk": (me + 1) % 16})

    order_first = (4, 5, 2, 3, 6, 7, 1)
    blk_first = (10, 9, 11, 6, 14, 8, 2, 5, 7, 13, 15, 1, 3, 4, 12)

    def pass_on(g):
        for d, source in pairs:
            wait_far(g, d, source)
            forward(g, d, source).start()

    def transform_group(g):
        all_near(g).wait_recv()
        side(g).wait_recv()
        all_forward(g).wait_recv()

        def butterfly(k, carry):
            rows = pl.ds(pl.multiple_of(16 * k, 16), 16)
            values = [xr[g, a // 4, rows, 128 * (a % 4):128 * (a % 4) + 128] for a in range(32)]
            result = real_dft(values)
            for r in range(16):
                pair = (result[0][0], result[16][0]) if r == 0 else result[r]
                for part, value in enumerate(pair):
                    top = value.astype(BF)
                    ycat[r, rows, 128 * part:128 * part + 128] = top
                    ycat[r, rows, 256 + 128 * part:384 + 128 * part] = (value - top.astype(F32)).astype(BF)
                    ycat[r, rows, 512 + 128 * part:640 + 128 * part] = top
            return carry

        lax.fori_loop(0, 4, butterfly, 0)

        for r in range(8):
            parts = [lax.dot_general(table[rr], ycat[rr], CONTRACT_LANES, preferred_element_type=F32) for rr in (r, r + 8)]
            both = jnp.concatenate(parts, axis=1)
            for o in range(8):
                rows = jnp.concatenate([both[8 * o:8 * o + 8], both[64 + 8 * o:64 + 8 * o + 8]], axis=0)
                terms[16 * r:16 * r + 16, 128 * o:128 * o + 128] = rows.astype(BF)
        part = jnp.dot(perm[...], terms[...], preferred_element_type=F32).astype(BF)
        for o in range(8):
            sbuf[g, o] = part[:, 128 * o:128 * o + 128].reshape(8, 16, 128)
        for piece in range(PIECES):
            for peer in order_first:
                exchange_order(g, piece, peer).start()
        srecv[g, order] = sbuf[g, order]

    def place_group(g, piece):
        all_order(g, piece).wait_recv()
        for tt in range(SPAN * piece, SPAN * piece + SPAN):
            parts = []
            for h in range(2):
                rows = srecv[g, :, 2 * tt + h].reshape(128, 128)
                out = lax.dot_general(place[...], rows, CONTRACT_LANES, preferred_element_type=F32)
                parts.append(out.reshape(16, 8, 128))
            sent[g, :, tt] = jnp.concatenate(parts, axis=1).astype(BF)
            arrived[g, me, tt] = sent[g, me, tt]
        for peer in blk_first:
            exchange_blk(g, piece, peer).start()

    def receive_group(g, piece):
        all_blk(g, piece).wait_recv()

    low_lanes = lax.broadcasted_iota(jnp.int32, (256, 128), 1) < 64

    def neighbour(axis, step):
        nx = (x + step * (1 - axis)) % 4
        nz = (z + step * axis) % 4
        return {"blk": nx * 4 + nz}

    def copies(s, kind, src, dst, axis):
        return [remote(src.at[s, way], dst.at[s, way], ring_s.at[s, kind], ring_r.at[s, kind],
                       neighbour(axis, 3 - 2 * way)) for way in range(2)]

    def ring(s, kind, src, dst):
        return remote(src.at[s], dst.at[s], ring_s.at[s, kind], ring_r.at[s, kind], {"blk": (me + 1) % 16})

    A, B = pl.ds(0, 128), pl.ds(128, 128)

    def compute(s):
        g, tt, par, qs = s // 4, s % 4, s % 2, s % 4

        if s < 4:
            pltpu.make_async_copy(leg.at[:, tt], leg.at[:, tt], leg_sem.at[tt]).wait()

        rows = lax.broadcasted_iota(jnp.int32, (256, 768), 0)
        lanes = lax.broadcasted_iota(jnp.int32, (256, 768), 1) % 16
        rh, mh = rows // 128, rows % 8
        swapped = (par == 1) & (mh > 0)
        mask = lanes == jnp.where(swapped, 8 - 8 * rh, 8 * rh) + mh
        values = arrived[g, :, tt].reshape(256, 128)
        lhs = []
        for h in range(2):
            ex = jnp.concatenate([
                lax.dot_general(values, expand[h, part], CONTRACT_ROWS, preferred_element_type=F32)
                for part in range(2)], axis=0)
            lhs.append(jnp.where(mask, ex, 0.0).astype(BF))
        for bx in range(4):
            pa, pb = [
                jnp.dot(lhs[h], leg[h, tt, :, :, 256 * bx:256 * bx + 256].reshape(768, 256),
                        preferred_element_type=F32)
                for h in range(2)
            ]
            for half in range(2):
                a = pa[:, 128 * half:128 * half + 128]
                b = pb[:, 128 * half:128 * half + 128]
                first = jnp.where(low_lanes, a, pltpu.roll(b, 64, 1))
                second = jnp.where(low_lanes, pltpu.roll(a, 64, 1), b)
                for bz, value in ((2 * half, first), (2 * half + 1, second)):
                    q[qs, bx * (1 - par) + bz * par, bz * (1 - par) + bx * par] = value
        i = x * (1 - par) + z * par
        c1, c2, c3 = (i + 1) % 4, (i + 2) % 4, (i + 3) % 4
        minus, plus = copies(s, 0, ms1, mr1, par)
        ms1[s, 0, 0] = q[qs, c2, :, A, :].astype(BF)
        ms1[s, 0, 1] = q[qs, c3, :, B, :].astype(BF)
        minus.start()
        ms1[s, 1, 0] = q[qs, c2, :, B, :].astype(BF)
        ms1[s, 1, 1] = q[qs, c1, :, A, :].astype(BF)
        plus.start()

    def relay1(s):
        par, qs = s % 2, s % 4
        i = x * (1 - par) + z * par
        c1, c3 = (i + 1) % 4, (i + 3) % 4
        send = copies(s, 1, ss1, sr1, par)
        ring(s, 0, ms1, mr1).wait_recv()
        ss1[s, 0] = (q[qs, c3, :, A, :] + mr1[s, 0, 0].astype(F32)).astype(BF)
        send[0].start()
        ss1[s, 1] = (q[qs, c1, :, B, :] + mr1[s, 1, 0].astype(F32)).astype(BF)
        send[1].start()

    def owner1(s):
        par, qs = s % 2, s % 4
        i = x * (1 - par) + z * par
        ring(s, 1, ss1, sr1).wait_recv()
        q2[s, :, A, :] = q[qs, i, :, A, :] + mr1[s, 1, 1].astype(F32) + sr1[s, 0].astype(F32)
        q2[s, :, B, :] = q[qs, i, :, B, :] + mr1[s, 0, 1].astype(F32) + sr1[s, 1].astype(F32)
        j = z * (1 - par) + x * par
        d1, d2, d3 = (j + 1) % 4, (j + 2) % 4, (j + 3) % 4
        ms2[s, 0, 0] = q2[s, d2, A, :].astype(BF)
        ms2[s, 0, 1] = q2[s, d3, B, :].astype(BF)
        ms2[s, 1, 0] = q2[s, d2, B, :].astype(BF)
        ms2[s, 1, 1] = q2[s, d1, A, :].astype(BF)
        for copy in copies(s, 2, ms2, mr2, 1 - par):
            copy.start()

    def relay2(s):
        par = s % 2
        j = z * (1 - par) + x * par
        d1, d3 = (j + 1) % 4, (j + 3) % 4
        send = copies(s, 3, ss2, sr2, 1 - par)
        ring(s, 2, ms2, mr2).wait_recv()
        ss2[s, 0] = (q2[s, d3, A, :] + mr2[s, 0, 0].astype(F32)).astype(BF)
        send[0].start()
        ss2[s, 1] = (q2[s, d1, B, :] + mr2[s, 1, 0].astype(F32)).astype(BF)
        send[1].start()

    def owner2(s):
        par = s % 2
        j = z * (1 - par) + x * par
        ring(s, 3, ss2, sr2).wait_recv()
        final[s, A, :] = q2[s, j, A, :] + mr2[s, 1, 1].astype(F32) + sr2[s, 0].astype(F32)
        final[s, B, :] = q2[s, j, B, :] + mr2[s, 0, 1].astype(F32) + sr2[s, 1].astype(F32)

    def output_group(g):
        top_row = lax.broadcasted_iota(jnp.int32, (8, 128), 0) == 0

        def column(fc, carry):
            pieces = []
            for tt in range(4):
                v0 = final[4 * g + tt, pl.ds(pl.multiple_of(8 * fc, 8), 8), :]
                v1 = final[4 * g + tt, pl.ds(pl.multiple_of(128 + 8 * fc, 8), 8), :]
                if tt % 2:
                    v0, v1 = jnp.where(top_row, v0, v1), jnp.where(top_row, v1, v0)
                pieces += [v0, v1]
            turned = jnp.concatenate(pieces, axis=0).T
            out_row = (fc // 2 * 2 + g) * 2 + fc % 2
            out_ref[pl.ds(out_row, 64, stride=32), :] = jnp.concatenate([turned[0:64], turned[64:128]], axis=1)
            return carry

        lax.fori_loop(0, 16, column, 0, unroll=4)

    def near_group(g):
        for d, other in pairs:
            near(g, d, other).start()

    def far_group(g):
        for d, other in pairs:
            far(g, d, other).start()

    def ring_drain(s, kinds):
        for kind in kinds:
            src, dst = ((ms1, mr1), (ss1, sr1), (ms2, mr2), (ss2, sr2))[kind]
            ring(s, kind, src, dst).wait_send()

    def drain_early():
        for g in range(2):
            all_far(g).wait_send()
            all_near(g).wait_send()
            all_forward(g).wait_send()
            side(g).wait_send()
            for piece in range(PIECES):
                all_order(g, piece).wait_send()
                all_blk(g, piece).wait_send()
        for s in range(4):
            ring_drain(s, (0, 1, 2, 3))
        for s in range(4, 8):
            ring_drain(s, (0,))

    def drain_late():
        for s in range(4, 8):
            ring_drain(s, (1, 2, 3))

    run = dict(F=far_group, N=near_group, P=pass_on, A=transform_group, B=place_group, C=receive_group, M=source_maps,
               m=compute, r=relay1, o=owner1, R=relay2, O=owner2, T=output_group, D=drain_early, E=drain_late)
    for name in SCHEDULE:
        run[name[0]](*map(int, name[1:]))


def analysis(field, mask, plan, legendre):
    high, low = dft_tables()
    vmem, anywhere = pl.BlockSpec(memory_space=pltpu.VMEM), pl.BlockSpec(memory_space=pl.ANY)
    dma = pltpu.SemaphoreType.DMA
    half = (NBLOCK, 2, 4, 128, 128)
    return pl.pallas_call(
        kernel,
        out_shape=pltpu.VMEM((2048, 128), F32),
        in_specs=[anywhere, anywhere, vmem, anywhere, anywhere, anywhere, anywhere],
        out_specs=vmem,
        scratch_shapes=[
            pltpu.VMEM((16, 64, 512), F32),
            pltpu.VMEM((64, 512), jnp.int32),
            pltpu.VMEM((16, 128, 768), BF), pltpu.VMEM((128, 128), BF),
            pltpu.VMEM((2, 8, 64, 512), F32),
            pltpu.VMEM((2, 2, 2, 32, 512), F32),
            pltpu.VMEM((16, 64, 768), BF),
            pltpu.VMEM((128, 1024), BF),
            pltpu.VMEM((2, 8, 8, 16, 128), BF), pltpu.VMEM((2, 8, 8, 16, 128), BF),
            pltpu.VMEM((128, 128), BF), pltpu.VMEM((2, 2, 256, 768), BF),
            pltpu.VMEM((2, 16, 4, 16, 128), BF), pltpu.VMEM((2, 16, 4, 16, 128), BF),
            pltpu.VMEM((2, 4, 48, 16, 1024), BF),
            pltpu.VMEM((4, 4, 4, 256, 128), F32),
            pltpu.VMEM((NBLOCK, 4, 256, 128), F32),
            pltpu.VMEM((NBLOCK, 2, 2, 4, 128, 128), BF), pltpu.VMEM((NBLOCK, 2, 2, 4, 128, 128), BF),
            pltpu.VMEM(half, BF), pltpu.VMEM(half, BF),
            pltpu.VMEM((NBLOCK, 2, 2, 128, 128), BF), pltpu.VMEM((NBLOCK, 2, 2, 128, 128), BF),
            pltpu.VMEM((NBLOCK, 2, 128, 128), BF), pltpu.VMEM((NBLOCK, 2, 128, 128), BF),
            pltpu.VMEM((NBLOCK, 256, 128), F32),
            dma((2,)), dma((4,)), dma((4,)),
            dma((2,)), dma((2, 2, 2)), dma((2,)), dma((2,)), dma((2,)), dma((2,)), dma((2,)), dma((2,)),
            dma((2, PIECES)), dma((2, PIECES)), dma((2, PIECES)), dma((2, PIECES)),
            dma((NBLOCK, 4)), dma((NBLOCK, 4)),
        ],
        compiler_params=pltpu.CompilerParams(collective_id=0, has_side_effects=True, vmem_limit_bytes=62 * 2**20),
    )(field, mask, plan.reshape(8, 128), jnp.asarray(high), jnp.asarray(low), jnp.asarray(order_permutation()), legendre)


def body(field, ocean_mask, plan, legendre):
    return analysis(field, ocean_mask, plan, legendre).reshape(64, 16, 2, 128)


def solution(mesh):
    placed = (P(None, "blk", "order"), P("blk", "order"), P(), P("blk", "order", None))
    return jax.shard_map(
        body, mesh=mesh, in_specs=placed, out_specs=P("blk", None, None, "order"), check_vma=False
    )
```

```python
import math

import jax
import jax.numpy as jnp
import numpy as np
from jax import lax
from jax.experimental import pallas as pl
from jax.experimental.pallas import tpu as pltpu
from jax.sharding import PartitionSpec as P

NLON = 4096
MESH = pl.DeviceIdType.MESH
BF = jnp.bfloat16
F32 = jnp.float32
NBLOCK = 8
CONTRACT_LANES = (((1,), (1,)), ((), ()))
CONTRACT_ROWS = (((0,), (0,)), ((), ()))

PIECES = 2
SPAN = 4 // PIECES
DIRECT = (6, 7)
SCHEDULE = (
    "P0", "F1", "M0", "A0", "N1", "P1", "B00", "B01", "C00", "m0", "m1", "C01", "A1", "m2", "m3", "r0", "B10", "B11",
    "r1", "r2", "o0", "r3", "o1", "C10", "m4", "C11", "m5", "o2", "m6", "o3", "m7", "R0", "R1", "r4", "r5", "R2",
    "R3", "r6", "r7", "o4", "o5", "O0", "O1", "O2", "O3", "T0", "o6", "o7", "R4", "R5", "D", "O4", "O5", "O6", "O7",
    "T1", "E",
)


def dft_tables():
    r = np.arange(16)[:, None, None]
    column = np.arange(64)[None, :, None]
    owner, w, ql = column // 8, column // 4 % 2, column % 4
    residue = np.where(w == 0, r, np.where(r == 0, 16, 32 - r))
    m = 32 * (4 * owner + ql) + residue
    i = np.arange(128)[None, None, :]
    angle = 2.0 * np.pi * (m * i % NLON) / NLON
    real, imag = np.cos(angle) / 64.0, np.where(w == 0, 1.0, -1.0) * np.sin(angle) / 64.0
    table = np.concatenate([real, imag], axis=2).astype(np.float32)
    high = table.astype(jnp.bfloat16)
    low = (table - high.astype(np.float32)).astype(jnp.bfloat16)
    return high, low


def order_permutation():
    out = np.zeros((128, 128), np.float32)
    for r in range(8):
        for w in range(2):
            for c in range(2):
                for ql in range(4):
                    mh = r if w == 0 else (8 - r) % 8
                    t = 2 * ql + w
                    out[(t % 4 * 2 + t // 4) * 16 + c * 8 + mh, r * 16 + c * 8 + w * 4 + ql] = 1.0
    return out.astype(jnp.bfloat16)


def real_dft(values):
    n = len(values)
    if n == 2:
        return [(values[0] + values[1], None), (values[0] - values[1], None)]
    even, odd = real_dft(values[0::2]), real_dft(values[1::2])
    half = n // 2

    def term(part, k):
        if k <= half // 2:
            return part[k]
        re, im = part[half - k]
        return re, (None if im is None else -im)

    result = [None] * (half + 1)
    for k in range(half // 2 + 1):
        er, ei = even[k]
        qr, qi = odd[k]
        cos, sin = math.cos(2 * math.pi * k / n), math.sin(2 * math.pi * k / n)
        if k == 0:
            result[0] = (er + qr, None)
            result[half] = (er - qr, None)
            continue
        if 4 * k == n:
            tr, ti = qi, -qr
        else:
            tr = qr * cos + qi * sin if qi is not None else qr * cos
            ti = qi * cos - qr * sin if qi is not None else -(qr * sin)

        def add(a, b, sign):
            if a is None:
                return None if b is None else (b if sign > 0 else -b)
            if b is None:
                return a
            return a + b if sign > 0 else a - b

        result[k] = (add(er, tr, 1), add(ei, ti, 1))
        if k != half - k:
            ni = add(ei, ti, -1)
            result[half - k] = (add(er, tr, -1), None if ni is None else -ni)
    return result


def kernel(field_hbm, mask_hbm, plan_ref, high_hbm, low_hbm, perm_hbm, leg_hbm, out_ref,
           masked, mask, table, perm, xr, relay, ycat, terms, sbuf, srecv, place, expand, sent, arrived,
           leg, q, q2, ms1, mr1, ss1, sr1, ms2, mr2, ss2, sr2, final,
           field_sem, load_sem, leg_sem, far_s, far_r, near_s, near_r, fwd_s, fwd_r, side_s, side_r,
           ox_s, ox_r, bx_s, bx_r, ring_s, ring_r):
    order = lax.axis_index("order")
    y, core = order // 2, order % 2
    me = lax.axis_index("blk")
    x, z = me // 4, me % 4

    def load_field(g, o):
        f = 2 * o + g
        return pltpu.make_async_copy(field_hbm.at[f], masked.at[f], field_sem.at[g])

    loads = [pltpu.make_async_copy(src, dst, load_sem.at[i]) for i, (src, dst) in enumerate(
        ((mask_hbm, mask), (high_hbm, table.at[:, pl.ds(0, 64), 0:256]),
         (low_hbm, table.at[:, pl.ds(0, 64), 512:768]), (perm_hbm, perm)))]

    def load_leg(t):
        return pltpu.make_async_copy(leg_hbm.at[:, pl.ds(16 * t, 16), :], leg.at[t // 4, t % 4], leg_sem.at[t % 4])

    loads[0].start()
    for o in range(8):
        load_field(0, o).start()

    barrier = pltpu.get_barrier_semaphore()
    order_peers = [(dy, dc) for dy in range(4) for dc in range(2) if (dy, dc) != (0, 0)]
    blk_peers = [(dx, dz) for dx in range(4) for dz in range(4) if (dx, dz) != (0, 0)]

    def at(dy, other):
        return {"order": (y + dy) % 4 * 2 + other}

    for dy, dc in order_peers:
        pl.semaphore_signal(barrier, inc=1, device_id=at(dy, (core + dc) % 2), device_id_type=MESH)
    for dx, dz in blk_peers:
        pl.semaphore_signal(barrier, inc=1, device_id={"blk": (x + dx) % 4 * 4 + (z + dz) % 4}, device_id_type=MESH)

    for o in range(8):
        load_field(1, o).start()
    for copy in loads[1:]:
        copy.start()
    loads[0].wait()

    def mask_fields(g):
        pltpu.make_async_copy(field_hbm.at[pl.ds(0, 8)], masked.at[pl.ds(0, 8)], field_sem.at[g]).wait()

        def one(o, carry):
            masked[2 * o + g] = masked[2 * o + g] * mask[...].astype(F32)
            return carry

        lax.fori_loop(0, 8, one, 0)
        xr[g, order] = masked[order * 2 + g]

    def remote(src, dst, ss, rs, device):
        return pltpu.make_async_remote_copy(src_ref=src, dst_ref=dst, send_sem=ss, recv_sem=rs,
                                            device_id=device, device_id_type=MESH)

    halves = (pl.ds(0, 32), pl.ds(32, 32))
    steps = (1, 3)
    pairs = [(d, other) for d in range(2) for other in range(2)]

    def far(g, d, other):
        target = ((y + 2) % 4 * 2 + other) * 2 + g
        return remote(masked.at[target, halves[d]], relay.at[g, d, core], far_s.at[g], far_r.at[g, d, core],
                      at(steps[d], other))

    def near(g, d, other):
        target = ((y + steps[d]) % 4 * 2 + other) * 2 + g
        return remote(masked.at[target], xr.at[g, order], near_s.at[g], near_r.at[g],
                      at(steps[d], other))

    def forward(g, d, source):
        origin = (y + 4 - steps[d]) % 4 * 2 + source
        return remote(relay.at[g, d, source], xr.at[g, origin, halves[d]], fwd_s.at[g], fwd_r.at[g],
                      at(steps[d], core))

    def side(g):
        target = (y * 2 + 1 - core) * 2 + g
        return remote(masked.at[target], xr.at[g, order], side_s.at[g], side_r.at[g], at(0, 1 - core))

    def wait_far(g, d, source):
        remote(masked.at[0, halves[d]], relay.at[g, d, source], far_s.at[g], far_r.at[g, d, source],
               at(steps[d], source)).wait_recv()

    def all_far(g):
        return remote(relay.at[g], relay.at[g], far_s.at[g], far_r.at[g, 0, 0], at(1, 0))

    def all_near(g):
        part = pl.ds(0, 4)
        return remote(xr.at[g, part], xr.at[g, part], near_s.at[g], near_r.at[g], at(1, 0))

    def all_forward(g):
        return remote(relay.at[g], relay.at[g], fwd_s.at[g], fwd_r.at[g], at(1, 0))

    mask_fields(0)
    pl.semaphore_wait(barrier, 22)
    for d, other in pairs:
        far(0, d, other).start()
    for d, other in pairs:
        near(0, d, other).start()
    side(0).start()
    for t in range(8):
        load_leg(t).start()
    mask_fields(1)
    side(1).start()

    earlier = (lax.broadcasted_iota(jnp.int32, (64, 64), 0) < lax.broadcasted_iota(jnp.int32, (64, 64), 1))
    earlier = earlier.astype(F32).astype(BF)

    def owner_of(b, rows):
        both = plan_ref[pl.ds(b // 2, 1), :]
        slots = jnp.broadcast_to(jnp.where(b % 2 == 0, both[:, 0:64], both[:, 64:128]), (rows, 64))
        owner = jnp.zeros((rows, 64), jnp.int32)
        for b in range(1, 17):
            owner += (slots >= 48 * b).astype(jnp.int32)
        return slots, owner

    def source_maps(_):
        row = lax.broadcasted_iota(jnp.int32, (128, 64), 0)
        _, owner = owner_of(me, 128)
        mine = owner == row // 8
        count = jnp.dot(mine.astype(F32).astype(BF), earlier, preferred_element_type=F32)
        match = mine & (count == (row // 2 % 4).astype(F32))
        for rh in range(2):
            place[:, 64 * rh:64 * rh + 64] = (match & (row % 2 == rh)).astype(F32).astype(BF)

        def source_map(b, carry):
            slots, owner = owner_of(b, 16)
            mine = owner == me
            count = jnp.dot(mine.astype(F32).astype(BF), earlier, preferred_element_type=F32)
            rows = lax.broadcasted_iota(jnp.int32, (16, 64), 0)
            match = mine & (count == (rows // 2 % 4).astype(F32))
            slot = jnp.sum(jnp.where(match, (slots - 48 * me + 1).astype(F32), 0.0), axis=1, keepdims=True)
            lanes = lax.broadcasted_iota(jnp.int32, (16, 768), 1) // 16 + 1
            rows = lax.broadcasted_iota(jnp.int32, (16, 768), 0)
            hit = jnp.broadcast_to(slot, (16, 768)) == lanes.astype(F32)
            for h in range(2):
                for rh in range(2):
                    expand[h, rh, pl.ds(pl.multiple_of(16 * b, 16), 16), :] = (
                        hit & (rows // 8 == h) & (rows % 2 == rh)).astype(F32).astype(BF)
            return carry

        lax.fori_loop(0, 16, source_map, 0)
        for copy in loads[1:]:
            copy.wait()

        w = lax.broadcasted_iota(jnp.int32, (64, 128), 0) // 4 % 2

        def complete(r, carry):
            for start in (0, 512):
                real = table[r, 0:64, start:start + 128].astype(F32)
                imag = table[r, 0:64, start + 128:start + 256].astype(F32)
                sign = jnp.where(w == 0, 1.0, -1.0)
                special = jnp.broadcast_to(r == 0, (64, 128))
                parts = (
                    (jnp.where(special & (w == 1), 0.0, real), jnp.where(special, jnp.where(w == 1, real, 0.0), imag)),
                    (jnp.where(special & (w == 1), 0.0, -sign * imag),
                     jnp.where(special, jnp.where(w == 1, imag, 0.0), sign * real)),
                )
                for c in range(2):
                    for half in range(2):
                        value = parts[c][half].astype(BF)
                        table[r, 64 * c:64 * c + 64, start + 128 * half:start + 128 * half + 128] = value
                        if start == 0:
                            table[r, 64 * c:64 * c + 64, 256 + 128 * half:384 + 128 * half] = value
            return carry

        lax.fori_loop(0, 16, complete, 0)

    def exchange_order(g, piece, peer):
        target = (y + peer // 2) % 4 * 2 + (core + peer) % 2
        rows = pl.ds(2 * SPAN * piece, 2 * SPAN)
        return remote(sbuf.at[g, target, rows], srecv.at[g, order, rows], ox_s.at[g, piece], ox_r.at[g, piece],
                      {"order": target})

    def exchange_blk(g, piece, peer):
        target = (x + peer // 4) % 4 * 4 + (z + peer) % 4
        rows = pl.ds(SPAN * piece, SPAN)
        return remote(sent.at[g, target, rows], arrived.at[g, me, rows], bx_s.at[g, piece], bx_r.at[g, piece],
                      {"blk": target})

    def all_order(g, piece):
        part = srecv.at[g, pl.ds(0, 7), pl.ds(2 * SPAN * piece, 2 * SPAN)]
        return remote(part, part, ox_s.at[g, piece], ox_r.at[g, piece], at(1, 0))

    def all_blk(g, piece):
        part = arrived.at[g, pl.ds(0, 15), pl.ds(SPAN * piece, SPAN)]
        return remote(part, part, bx_s.at[g, piece], bx_r.at[g, piece], {"blk": (me + 1) % 16})

    order_first = (4, 5, 2, 3, 6, 7, 1)
    blk_first = (10, 9, 11, 6, 14, 8, 2, 5, 7, 13, 15, 1, 3, 4, 12)

    def pass_on(g):
        for d, source in pairs:
            wait_far(g, d, source)
            forward(g, d, source).start()

    def transform_group(g):
        all_near(g).wait_recv()
        side(g).wait_recv()
        all_forward(g).wait_recv()

        def butterfly(k, carry):
            rows = pl.ds(pl.multiple_of(16 * k, 16), 16)
            values = [xr[g, a // 4, rows, 128 * (a % 4):128 * (a % 4) + 128] for a in range(32)]
            result = real_dft(values)
            for r in range(16):
                pair = (result[0][0], result[16][0]) if r == 0 else result[r]
                for part, value in enumerate(pair):
                    top = value.astype(BF)
                    ycat[r, rows, 128 * part:128 * part + 128] = top
                    ycat[r, rows, 256 + 128 * part:384 + 128 * part] = (value - top.astype(F32)).astype(BF)
                    ycat[r, rows, 512 + 128 * part:640 + 128 * part] = top
            return carry

        lax.fori_loop(0, 4, butterfly, 0)

        for r in range(8):
            parts = [lax.dot_general(table[rr], ycat[rr], CONTRACT_LANES, preferred_element_type=F32) for rr in (r, r + 8)]
            both = jnp.concatenate(parts, axis=1)
            for o in range(8):
                rows = jnp.concatenate([both[8 * o:8 * o + 8], both[64 + 8 * o:64 + 8 * o + 8]], axis=0)
                terms[16 * r:16 * r + 16, 128 * o:128 * o + 128] = rows.astype(BF)
        part = jnp.dot(perm[...], terms[...], preferred_element_type=F32).astype(BF)
        for o in range(8):
            sbuf[g, o] = part[:, 128 * o:128 * o + 128].reshape(8, 16, 128)
        for piece in range(PIECES):
            for peer in order_first:
                exchange_order(g, piece, peer).start()
        srecv[g, order] = sbuf[g, order]

    def place_group(g, piece):
        all_order(g, piece).wait_recv()
        for tt in range(SPAN * piece, SPAN * piece + SPAN):
            parts = []
            for h in range(2):
                rows = srecv[g, :, 2 * tt + h].reshape(128, 128)
                out = lax.dot_general(place[...], rows, CONTRACT_LANES, preferred_element_type=F32)
                parts.append(out.reshape(16, 8, 128))
            sent[g, :, tt] = jnp.concatenate(parts, axis=1).astype(BF)
            arrived[g, me, tt] = sent[g, me, tt]
        for peer in blk_first:
            exchange_blk(g, piece, peer).start()

    def receive_group(g, piece):
        all_blk(g, piece).wait_recv()

    low_lanes = lax.broadcasted_iota(jnp.int32, (256, 128), 1) < 64

    def neighbour(axis, step):
        nx = (x + step * (1 - axis)) % 4
        nz = (z + step * axis) % 4
        return {"blk": nx * 4 + nz}

    def copies(s, kind, src, dst, axis):
        return [remote(src.at[s, way], dst.at[s, way], ring_s.at[s, kind], ring_r.at[s, kind],
                       neighbour(axis, 3 - 2 * way)) for way in range(2)]

    def ring(s, kind, src, dst):
        return remote(src.at[s], dst.at[s], ring_s.at[s, kind], ring_r.at[s, kind], {"blk": (me + 1) % 16})

    A, B = pl.ds(0, 128), pl.ds(128, 128)

    def compute(s):
        g, tt, par, qs = s // 4, s % 4, s % 2, s % 4

        if s < 4:
            pltpu.make_async_copy(leg.at[:, tt], leg.at[:, tt], leg_sem.at[tt]).wait()

        rows = lax.broadcasted_iota(jnp.int32, (256, 768), 0)
        lanes = lax.broadcasted_iota(jnp.int32, (256, 768), 1) % 16
        rh, mh = rows // 128, rows % 8
        swapped = (par == 1) & (mh > 0)
        mask = lanes == jnp.where(swapped, 8 - 8 * rh, 8 * rh) + mh
        values = arrived[g, :, tt].reshape(256, 128)
        lhs = []
        for h in range(2):
            ex = jnp.concatenate([
                lax.dot_general(values, expand[h, part], CONTRACT_ROWS, preferred_element_type=F32)
                for part in range(2)], axis=0)
            lhs.append(jnp.where(mask, ex, 0.0).astype(BF))
        for bx in range(4):
            pa, pb = [
                jnp.dot(lhs[h], leg[h, tt, :, :, 256 * bx:256 * bx + 256].reshape(768, 256),
                        preferred_element_type=F32)
                for h in range(2)
            ]
            for half in range(2):
                a = pa[:, 128 * half:128 * half + 128]
                b = pb[:, 128 * half:128 * half + 128]
                first = jnp.where(low_lanes, a, pltpu.roll(b, 64, 1))
                second = jnp.where(low_lanes, pltpu.roll(a, 64, 1), b)
                for bz, value in ((2 * half, first), (2 * half + 1, second)):
                    q[qs, bx * (1 - par) + bz * par, bz * (1 - par) + bx * par] = value
        i = x * (1 - par) + z * par
        c1, c2, c3 = (i + 1) % 4, (i + 2) % 4, (i + 3) % 4
        minus, plus = copies(s, 0, ms1, mr1, par)
        ms1[s, 0, 0] = q[qs, c2, :, A, :].astype(BF)
        ms1[s, 0, 1] = q[qs, c3, :, B, :].astype(BF)
        minus.start()
        ms1[s, 1, 0] = q[qs, c2, :, B, :].astype(BF)
        ms1[s, 1, 1] = q[qs, c1, :, A, :].astype(BF)
        plus.start()

    def relay1(s):
        par, qs = s % 2, s % 4
        i = x * (1 - par) + z * par
        c1, c3 = (i + 1) % 4, (i + 3) % 4
        send = copies(s, 1, ss1, sr1, par)
        ring(s, 0, ms1, mr1).wait_recv()
        ss1[s, 0] = (q[qs, c3, :, A, :] + mr1[s, 0, 0].astype(F32)).astype(BF)
        send[0].start()
        ss1[s, 1] = (q[qs, c1, :, B, :] + mr1[s, 1, 0].astype(F32)).astype(BF)
        send[1].start()

    def owner1(s):
        par, qs = s % 2, s % 4
        i = x * (1 - par) + z * par
        ring(s, 1, ss1, sr1).wait_recv()
        q2[s, :, A, :] = q[qs, i, :, A, :] + mr1[s, 1, 1].astype(F32) + sr1[s, 0].astype(F32)
        q2[s, :, B, :] = q[qs, i, :, B, :] + mr1[s, 0, 1].astype(F32) + sr1[s, 1].astype(F32)
        j = z * (1 - par) + x * par
        d1, d2, d3 = (j + 1) % 4, (j + 2) % 4, (j + 3) % 4
        if s in DIRECT:
            ss2[s] = q2[s, d2].reshape(2, 128, 128).astype(BF)
            remote(ss2.at[s], sr2.at[s], ring_s.at[s, 3], ring_r.at[s, 3], neighbour(1 - par, 2)).start()
            ms2[s, 0] = q2[s, d3].reshape(2, 128, 128).astype(BF)
            ms2[s, 1] = q2[s, d1].reshape(2, 128, 128).astype(BF)
            for copy in copies(s, 2, ms2, mr2, 1 - par):
                copy.start()
            return
        ms2[s, 0, 0] = q2[s, d2, A, :].astype(BF)
        ms2[s, 0, 1] = q2[s, d3, B, :].astype(BF)
        ms2[s, 1, 0] = q2[s, d2, B, :].astype(BF)
        ms2[s, 1, 1] = q2[s, d1, A, :].astype(BF)
        for copy in copies(s, 2, ms2, mr2, 1 - par):
            copy.start()

    def relay2(s):
        par = s % 2
        j = z * (1 - par) + x * par
        d1, d3 = (j + 1) % 4, (j + 3) % 4
        send = copies(s, 3, ss2, sr2, 1 - par)
        ring(s, 2, ms2, mr2).wait_recv()
        ss2[s, 0] = (q2[s, d3, A, :] + mr2[s, 0, 0].astype(F32)).astype(BF)
        send[0].start()
        ss2[s, 1] = (q2[s, d1, B, :] + mr2[s, 1, 0].astype(F32)).astype(BF)
        send[1].start()

    def owner2(s):
        par = s % 2
        j = z * (1 - par) + x * par
        if s in DIRECT:
            ring(s, 2, ms2, mr2).wait_recv()
            ring(s, 3, ss2, sr2).wait_recv()
            total = mr2[s, 0].astype(F32) + mr2[s, 1].astype(F32) + sr2[s].astype(F32)
            final[s] = q2[s, j] + total.reshape(256, 128)
            return
        ring(s, 3, ss2, sr2).wait_recv()
        final[s, A, :] = q2[s, j, A, :] + mr2[s, 1, 1].astype(F32) + sr2[s, 0].astype(F32)
        final[s, B, :] = q2[s, j, B, :] + mr2[s, 0, 1].astype(F32) + sr2[s, 1].astype(F32)

    def output_group(g):
        top_row = lax.broadcasted_iota(jnp.int32, (8, 128), 0) == 0

        def column(fc, carry):
            pieces = []
            for tt in range(4):
                v0 = final[4 * g + tt, pl.ds(pl.multiple_of(8 * fc, 8), 8), :]
                v1 = final[4 * g + tt, pl.ds(pl.multiple_of(128 + 8 * fc, 8), 8), :]
                if tt % 2:
                    v0, v1 = jnp.where(top_row, v0, v1), jnp.where(top_row, v1, v0)
                pieces += [v0, v1]
            turned = jnp.concatenate(pieces, axis=0).T
            out_row = (fc // 2 * 2 + g) * 2 + fc % 2
            out_ref[pl.ds(out_row, 64, stride=32), :] = jnp.concatenate([turned[0:64], turned[64:128]], axis=1)
            return carry

        lax.fori_loop(0, 16, column, 0, unroll=16)

    def near_group(g):
        for d, other in pairs:
            near(g, d, other).start()

    def far_group(g):
        for d, other in pairs:
            far(g, d, other).start()

    def ring_drain(s, kinds):
        for kind in kinds:
            src, dst = ((ms1, mr1), (ss1, sr1), (ms2, mr2), (ss2, sr2))[kind]
            ring(s, kind, src, dst).wait_send()

    def drain_early():
        for g in range(2):
            all_far(g).wait_send()
            all_near(g).wait_send()
            all_forward(g).wait_send()
            side(g).wait_send()
            for piece in range(PIECES):
                all_order(g, piece).wait_send()
                all_blk(g, piece).wait_send()
        for s in range(4):
            ring_drain(s, (0, 1, 2, 3))
        for s in range(4, 8):
            ring_drain(s, (0,))

    def drain_late():
        for s in range(4, 8):
            ring_drain(s, (1, 2, 3))

    run = dict(F=far_group, N=near_group, P=pass_on, A=transform_group, B=place_group, C=receive_group, M=source_maps,
               m=compute, r=relay1, o=owner1, R=relay2, O=owner2, T=output_group, D=drain_early, E=drain_late)
    for name in SCHEDULE:
        run[name[0]](*map(int, name[1:]))


def analysis(field, mask, plan, legendre):
    high, low = dft_tables()
    vmem, anywhere = pl.BlockSpec(memory_space=pltpu.VMEM), pl.BlockSpec(memory_space=pl.ANY)
    dma = pltpu.SemaphoreType.DMA
    half = (NBLOCK, 2, 4, 128, 128)
    return pl.pallas_call(
        kernel,
        out_shape=pltpu.VMEM((2048, 128), F32),
        in_specs=[anywhere, anywhere, vmem, anywhere, anywhere, anywhere, anywhere],
        out_specs=vmem,
        scratch_shapes=[
            pltpu.VMEM((16, 64, 512), F32),
            pltpu.VMEM((64, 512), jnp.int32),
            pltpu.VMEM((16, 128, 768), BF), pltpu.VMEM((128, 128), BF),
            pltpu.VMEM((2, 8, 64, 512), F32),
            pltpu.VMEM((2, 2, 2, 32, 512), F32),
            pltpu.VMEM((16, 64, 768), BF),
            pltpu.VMEM((128, 1024), BF),
            pltpu.VMEM((2, 8, 8, 16, 128), BF), pltpu.VMEM((2, 8, 8, 16, 128), BF),
            pltpu.VMEM((128, 128), BF), pltpu.VMEM((2, 2, 256, 768), BF),
            pltpu.VMEM((2, 16, 4, 16, 128), BF), pltpu.VMEM((2, 16, 4, 16, 128), BF),
            pltpu.VMEM((2, 4, 48, 16, 1024), BF),
            pltpu.VMEM((4, 4, 4, 256, 128), F32),
            pltpu.VMEM((NBLOCK, 4, 256, 128), F32),
            pltpu.VMEM((NBLOCK, 2, 2, 4, 128, 128), BF), pltpu.VMEM((NBLOCK, 2, 2, 4, 128, 128), BF),
            pltpu.VMEM(half, BF), pltpu.VMEM(half, BF),
            pltpu.VMEM((NBLOCK, 2, 2, 128, 128), BF), pltpu.VMEM((NBLOCK, 2, 2, 128, 128), BF),
            pltpu.VMEM((NBLOCK, 2, 128, 128), BF), pltpu.VMEM((NBLOCK, 2, 128, 128), BF),
            pltpu.VMEM((NBLOCK, 256, 128), F32),
            dma((2,)), dma((4,)), dma((4,)),
            dma((2,)), dma((2, 2, 2)), dma((2,)), dma((2,)), dma((2,)), dma((2,)), dma((2,)), dma((2,)),
            dma((2, PIECES)), dma((2, PIECES)), dma((2, PIECES)), dma((2, PIECES)),
            dma((NBLOCK, 4)), dma((NBLOCK, 4)),
        ],
        compiler_params=pltpu.CompilerParams(collective_id=0, has_side_effects=True, vmem_limit_bytes=62 * 2**20),
    )(field, mask, plan.reshape(8, 128), jnp.asarray(high), jnp.asarray(low), jnp.asarray(order_permutation()), legendre)


def body(field, ocean_mask, plan, legendre):
    return analysis(field, ocean_mask, plan, legendre).reshape(64, 16, 2, 128)


def solution(mesh):
    placed = (P(None, "blk", "order"), P("blk", "order"), P(), P("blk", "order", None))
    return jax.shard_map(
        body, mesh=mesh, in_specs=placed, out_specs=P("blk", None, None, "order"), check_vma=False
    )
```

```python
import math

import jax
import jax.numpy as jnp
import numpy as np
from jax import lax
from jax.experimental import pallas as pl
from jax.experimental.pallas import tpu as pltpu
from jax.sharding import PartitionSpec as P

NLON = 4096
MESH = pl.DeviceIdType.MESH
BF = jnp.bfloat16
F32 = jnp.float32
NBLOCK = 8
CONTRACT_LANES = (((1,), (1,)), ((), ()))
CONTRACT_ROWS = (((0,), (0,)), ((), ()))

PIECES = 2
SPAN = 4 // PIECES
DIRECT = (6, 7)
SCHEDULE = (
    "P0", "F1", "M0", "A0", "N1", "P1", "B00", "B01", "C00", "m0", "m1", "C01", "A1", "m2", "m3", "r0", "B10", "B11",
    "r1", "r2", "o0", "r3", "o1", "C10", "m4", "C11", "m5", "o2", "m6", "o3", "m7", "R0", "R1", "r4", "r5", "R2",
    "R3", "r6", "r7", "o4", "o5", "O0", "O1", "O2", "O3", "T0", "o6", "o7", "R4", "R5", "D", "O4", "O5", "O6", "O7",
    "T1", "E",
)


def dft_tables():
    r = np.arange(16)[:, None, None]
    column = np.arange(64)[None, :, None]
    owner, w, ql = column // 8, column // 4 % 2, column % 4
    residue = np.where(w == 0, r, np.where(r == 0, 16, 32 - r))
    m = 32 * (4 * owner + ql) + residue
    i = np.arange(128)[None, None, :]
    angle = 2.0 * np.pi * (m * i % NLON) / NLON
    real, imag = np.cos(angle) / 64.0, np.where(w == 0, 1.0, -1.0) * np.sin(angle) / 64.0
    table = np.concatenate([real, imag], axis=2).astype(np.float32)
    high = table.astype(jnp.bfloat16)
    low = (table - high.astype(np.float32)).astype(jnp.bfloat16)
    return high, low


def order_permutation():
    out = np.zeros((128, 128), np.float32)
    for r in range(8):
        for w in range(2):
            for c in range(2):
                for ql in range(4):
                    mh = r if w == 0 else (8 - r) % 8
                    t = 2 * ql + w
                    out[(t % 4 * 2 + t // 4) * 16 + c * 8 + mh, r * 16 + c * 8 + w * 4 + ql] = 1.0
    return out.astype(jnp.bfloat16)


def real_dft(values):
    n = len(values)
    if n == 2:
        return [(values[0] + values[1], None), (values[0] - values[1], None)]
    even, odd = real_dft(values[0::2]), real_dft(values[1::2])
    half = n // 2

    def term(part, k):
        if k <= half // 2:
            return part[k]
        re, im = part[half - k]
        return re, (None if im is None else -im)

    result = [None] * (half + 1)
    for k in range(half // 2 + 1):
        er, ei = even[k]
        qr, qi = odd[k]
        cos, sin = math.cos(2 * math.pi * k / n), math.sin(2 * math.pi * k / n)
        if k == 0:
            result[0] = (er + qr, None)
            result[half] = (er - qr, None)
            continue
        if 4 * k == n:
            tr, ti = qi, -qr
        else:
            tr = qr * cos + qi * sin if qi is not None else qr * cos
            ti = qi * cos - qr * sin if qi is not None else -(qr * sin)

        def add(a, b, sign):
            if a is None:
                return None if b is None else (b if sign > 0 else -b)
            if b is None:
                return a
            return a + b if sign > 0 else a - b

        result[k] = (add(er, tr, 1), add(ei, ti, 1))
        if k != half - k:
            ni = add(ei, ti, -1)
            result[half - k] = (add(er, tr, -1), None if ni is None else -ni)
    return result


def kernel(field_hbm, mask_hbm, plan_ref, high_hbm, low_hbm, perm_hbm, leg_hbm, out_ref,
           masked, mask, table, perm, xr, relay, ycat, terms, sbuf, srecv, place, expand, sent, arrived,
           leg, q, q2, ms1, mr1, ss1, sr1, ms2, mr2, ss2, sr2, final,
           field_sem, load_sem, leg_sem, far_s, far_r, near_s, near_r, fwd_s, fwd_r, side_s, side_r,
           ox_s, ox_r, bx_s, bx_r, ring_s, ring_r):
    order = lax.axis_index("order")
    y, core = order // 2, order % 2
    me = lax.axis_index("blk")
    x, z = me // 4, me % 4

    def load_field(g, o):
        f = 2 * o + g
        return pltpu.make_async_copy(field_hbm.at[f], masked.at[f], field_sem.at[g])

    loads = [pltpu.make_async_copy(src, dst, load_sem.at[i]) for i, (src, dst) in enumerate(
        ((mask_hbm, mask), (high_hbm, table.at[:, pl.ds(0, 64), 0:256]),
         (low_hbm, table.at[:, pl.ds(0, 64), 512:768]), (perm_hbm, perm)))]

    def load_leg(t):
        return pltpu.make_async_copy(leg_hbm.at[:, pl.ds(16 * t, 16), :], leg.at[t // 4, t % 4], leg_sem.at[t % 4])

    loads[0].start()
    for o in range(8):
        load_field(0, o).start()

    barrier = pltpu.get_barrier_semaphore()
    order_peers = [(dy, dc) for dy in range(4) for dc in range(2) if (dy, dc) != (0, 0)]
    blk_peers = [(dx, dz) for dx in range(4) for dz in range(4) if (dx, dz) != (0, 0)]

    def at(dy, other):
        return {"order": (y + dy) % 4 * 2 + other}

    for dy, dc in order_peers:
        pl.semaphore_signal(barrier, inc=1, device_id=at(dy, (core + dc) % 2), device_id_type=MESH)
    for dx, dz in blk_peers:
        pl.semaphore_signal(barrier, inc=1, device_id={"blk": (x + dx) % 4 * 4 + (z + dz) % 4}, device_id_type=MESH)

    for o in range(8):
        load_field(1, o).start()
    for copy in loads[1:]:
        copy.start()
    loads[0].wait()

    def mask_fields(g):
        pltpu.make_async_copy(field_hbm.at[pl.ds(0, 8)], masked.at[pl.ds(0, 8)], field_sem.at[g]).wait()

        def one(o, carry):
            masked[2 * o + g] = masked[2 * o + g] * mask[...].astype(F32)
            return carry

        lax.fori_loop(0, 8, one, 0)
        xr[g, order] = masked[order * 2 + g]

    def remote(src, dst, ss, rs, device):
        return pltpu.make_async_remote_copy(src_ref=src, dst_ref=dst, send_sem=ss, recv_sem=rs,
                                            device_id=device, device_id_type=MESH)

    halves = (pl.ds(0, 32), pl.ds(32, 32))
    steps = (1, 3)
    pairs = [(d, other) for d in range(2) for other in range(2)]

    def far(g, d, other):
        target = ((y + 2) % 4 * 2 + other) * 2 + g
        return remote(masked.at[target, halves[d]], relay.at[g, d, core], far_s.at[g], far_r.at[g, d, core],
                      at(steps[d], other))

    def near(g, d, other):
        target = ((y + steps[d]) % 4 * 2 + other) * 2 + g
        return remote(masked.at[target], xr.at[g, order], near_s.at[g], near_r.at[g],
                      at(steps[d], other))

    def forward(g, d, source):
        origin = (y + 4 - steps[d]) % 4 * 2 + source
        return remote(relay.at[g, d, source], xr.at[g, origin, halves[d]], fwd_s.at[g], fwd_r.at[g],
                      at(steps[d], core))

    def side(g):
        target = (y * 2 + 1 - core) * 2 + g
        return remote(masked.at[target], xr.at[g, order], side_s.at[g], side_r.at[g], at(0, 1 - core))

    def wait_far(g, d, source):
        remote(masked.at[0, halves[d]], relay.at[g, d, source], far_s.at[g], far_r.at[g, d, source],
               at(steps[d], source)).wait_recv()

    def all_far(g):
        return remote(relay.at[g], relay.at[g], far_s.at[g], far_r.at[g, 0, 0], at(1, 0))

    def all_near(g):
        part = pl.ds(0, 4)
        return remote(xr.at[g, part], xr.at[g, part], near_s.at[g], near_r.at[g], at(1, 0))

    def all_forward(g):
        return remote(relay.at[g], relay.at[g], fwd_s.at[g], fwd_r.at[g], at(1, 0))

    mask_fields(0)
    pl.semaphore_wait(barrier, 22)
    for d, other in pairs:
        far(0, d, other).start()
    for d, other in pairs:
        near(0, d, other).start()
    side(0).start()
    for t in range(8):
        load_leg(t).start()
    mask_fields(1)
    side(1).start()

    earlier = (lax.broadcasted_iota(jnp.int32, (64, 64), 0) < lax.broadcasted_iota(jnp.int32, (64, 64), 1))
    earlier = earlier.astype(F32).astype(BF)

    def owner_of(b, rows):
        both = plan_ref[pl.ds(b // 2, 1), :]
        slots = jnp.broadcast_to(jnp.where(b % 2 == 0, both[:, 0:64], both[:, 64:128]), (rows, 64))
        owner = jnp.zeros((rows, 64), jnp.int32)
        for b in range(1, 17):
            owner += (slots >= 48 * b).astype(jnp.int32)
        return slots, owner

    def source_maps(_):
        row = lax.broadcasted_iota(jnp.int32, (128, 64), 0)
        _, owner = owner_of(me, 128)
        mine = owner == row // 8
        count = jnp.dot(mine.astype(F32).astype(BF), earlier, preferred_element_type=F32)
        match = mine & (count == (row // 2 % 4).astype(F32))
        for rh in range(2):
            place[:, 64 * rh:64 * rh + 64] = (match & (row % 2 == rh)).astype(F32).astype(BF)

        def source_map(b, carry):
            slots, owner = owner_of(b, 16)
            mine = owner == me
            count = jnp.dot(mine.astype(F32).astype(BF), earlier, preferred_element_type=F32)
            rows = lax.broadcasted_iota(jnp.int32, (16, 64), 0)
            match = mine & (count == (rows // 2 % 4).astype(F32))
            slot = jnp.sum(jnp.where(match, (slots - 48 * me + 1).astype(F32), 0.0), axis=1, keepdims=True)
            lanes = lax.broadcasted_iota(jnp.int32, (16, 768), 1) // 16 + 1
            rows = lax.broadcasted_iota(jnp.int32, (16, 768), 0)
            hit = jnp.broadcast_to(slot, (16, 768)) == lanes.astype(F32)
            for h in range(2):
                for rh in range(2):
                    expand[h, rh, pl.ds(pl.multiple_of(16 * b, 16), 16), :] = (
                        hit & (rows // 8 == h) & (rows % 2 == rh)).astype(F32).astype(BF)
            return carry

        lax.fori_loop(0, 16, source_map, 0)
        for copy in loads[1:]:
            copy.wait()

        w = lax.broadcasted_iota(jnp.int32, (64, 128), 0) // 4 % 2

        def complete(r, carry):
            for start in (0, 512):
                real = table[r, 0:64, start:start + 128].astype(F32)
                imag = table[r, 0:64, start + 128:start + 256].astype(F32)
                sign = jnp.where(w == 0, 1.0, -1.0)
                special = jnp.broadcast_to(r == 0, (64, 128))
                parts = (
                    (jnp.where(special & (w == 1), 0.0, real), jnp.where(special, jnp.where(w == 1, real, 0.0), imag)),
                    (jnp.where(special & (w == 1), 0.0, -sign * imag),
                     jnp.where(special, jnp.where(w == 1, imag, 0.0), sign * real)),
                )
                for c in range(2):
                    for half in range(2):
                        value = parts[c][half].astype(BF)
                        table[r, 64 * c:64 * c + 64, start + 128 * half:start + 128 * half + 128] = value
                        if start == 0:
                            table[r, 64 * c:64 * c + 64, 256 + 128 * half:384 + 128 * half] = value
            return carry

        lax.fori_loop(0, 16, complete, 0)

    def exchange_order(g, piece, peer):
        target = (y + peer // 2) % 4 * 2 + (core + peer) % 2
        rows = pl.ds(2 * SPAN * piece, 2 * SPAN)
        return remote(sbuf.at[g, target, rows], srecv.at[g, order, rows], ox_s.at[g, piece], ox_r.at[g, piece],
                      {"order": target})

    def exchange_blk(g, piece, peer):
        target = (x + peer // 4) % 4 * 4 + (z + peer) % 4
        rows = pl.ds(SPAN * piece, SPAN)
        return remote(sent.at[g, target, rows], arrived.at[g, me, rows], bx_s.at[g, piece], bx_r.at[g, piece],
                      {"blk": target})

    def all_order(g, piece):
        part = srecv.at[g, pl.ds(0, 7), pl.ds(2 * SPAN * piece, 2 * SPAN)]
        return remote(part, part, ox_s.at[g, piece], ox_r.at[g, piece], at(1, 0))

    def all_blk(g, piece):
        part = arrived.at[g, pl.ds(0, 15), pl.ds(SPAN * piece, SPAN)]
        return remote(part, part, bx_s.at[g, piece], bx_r.at[g, piece], {"blk": (me + 1) % 16})

    order_first = (4, 5, 2, 3, 6, 7, 1)
    blk_first = (10, 9, 11, 6, 14, 8, 2, 5, 7, 13, 15, 1, 3, 4, 12)

    def pass_on(g):
        for d, source in pairs:
            wait_far(g, d, source)
            forward(g, d, source).start()

    def transform_group(g):
        all_near(g).wait_recv()
        side(g).wait_recv()
        all_forward(g).wait_recv()

        def butterfly(k, carry):
            rows = pl.ds(pl.multiple_of(16 * k, 16), 16)
            values = [xr[g, a // 4, rows, 128 * (a % 4):128 * (a % 4) + 128] for a in range(32)]
            result = real_dft(values)
            for r in range(16):
                pair = (result[0][0], result[16][0]) if r == 0 else result[r]
                for part, value in enumerate(pair):
                    top = value.astype(BF)
                    ycat[r, rows, 128 * part:128 * part + 128] = top
                    ycat[r, rows, 256 + 128 * part:384 + 128 * part] = (value - top.astype(F32)).astype(BF)
                    ycat[r, rows, 512 + 128 * part:640 + 128 * part] = top
            return carry

        lax.fori_loop(0, 4, butterfly, 0)

        for r in range(8):
            parts = [lax.dot_general(table[rr], ycat[rr], CONTRACT_LANES, preferred_element_type=F32) for rr in (r, r + 8)]
            both = jnp.concatenate(parts, axis=1)
            for o in range(8):
                rows = jnp.concatenate([both[8 * o:8 * o + 8], both[64 + 8 * o:64 + 8 * o + 8]], axis=0)
                terms[16 * r:16 * r + 16, 128 * o:128 * o + 128] = rows.astype(BF)
        part = jnp.dot(perm[...], terms[...], preferred_element_type=F32).astype(BF)
        for o in range(8):
            sbuf[g, o] = part[:, 128 * o:128 * o + 128].reshape(8, 16, 128)
        for piece in range(PIECES):
            for peer in order_first:
                exchange_order(g, piece, peer).start()
        srecv[g, order] = sbuf[g, order]

    def place_group(g, piece):
        all_order(g, piece).wait_recv()
        for tt in range(SPAN * piece, SPAN * piece + SPAN):
            parts = []
            for h in range(2):
                rows = srecv[g, :, 2 * tt + h].reshape(128, 128)
                out = lax.dot_general(place[...], rows, CONTRACT_LANES, preferred_element_type=F32)
                parts.append(out.reshape(16, 8, 128))
            sent[g, :, tt] = jnp.concatenate(parts, axis=1).astype(BF)
            arrived[g, me, tt] = sent[g, me, tt]
        for peer in blk_first:
            exchange_blk(g, piece, peer).start()

    def receive_group(g, piece):
        all_blk(g, piece).wait_recv()

    low_lanes = lax.broadcasted_iota(jnp.int32, (256, 128), 1) < 64

    def neighbour(axis, step):
        nx = (x + step * (1 - axis)) % 4
        nz = (z + step * axis) % 4
        return {"blk": nx * 4 + nz}

    def copies(s, kind, src, dst, axis):
        return [remote(src.at[s, way], dst.at[s, way], ring_s.at[s, kind], ring_r.at[s, kind],
                       neighbour(axis, 3 - 2 * way)) for way in range(2)]

    def ring(s, kind, src, dst):
        return remote(src.at[s], dst.at[s], ring_s.at[s, kind], ring_r.at[s, kind], {"blk": (me + 1) % 16})

    A, B = pl.ds(0, 128), pl.ds(128, 128)

    def compute(s):
        g, tt, par, qs = s // 4, s % 4, s % 2, s % 4

        if s < 4:
            pltpu.make_async_copy(leg.at[:, tt], leg.at[:, tt], leg_sem.at[tt]).wait()

        rows = lax.broadcasted_iota(jnp.int32, (256, 768), 0)
        lanes = lax.broadcasted_iota(jnp.int32, (256, 768), 1) % 16
        rh, mh = rows // 128, rows % 8
        swapped = (par == 1) & (mh > 0)
        mask = lanes == jnp.where(swapped, 8 - 8 * rh, 8 * rh) + mh
        values = arrived[g, :, tt].reshape(256, 128)
        lhs = []
        for h in range(2):
            ex = jnp.concatenate([
                lax.dot_general(values, expand[h, part], CONTRACT_ROWS, preferred_element_type=F32)
                for part in range(2)], axis=0)
            lhs.append(jnp.where(mask, ex, 0.0).astype(BF))
        i = x * (1 - par) + z * par
        c1, c2, c3 = (i + 1) % 4, (i + 2) % 4, (i + 3) % 4
        minus, plus = copies(s, 0, ms1, mr1, par)

        def send_minus():
            ms1[s, 0, 0] = q[qs, c2, :, A, :].astype(BF)
            ms1[s, 0, 1] = q[qs, c3, :, B, :].astype(BF)
            minus.start()

        def send_plus():
            ms1[s, 1, 0] = q[qs, c2, :, B, :].astype(BF)
            ms1[s, 1, 1] = q[qs, c1, :, A, :].astype(BF)
            plus.start()

        for bx in ((c2, c3, c1, i) if s == 0 else range(4)):
            lanes = pl.ds(pl.multiple_of(256 * bx, 256), 256) if s == 0 else pl.ds(256 * bx, 256)
            pa, pb = [
                jnp.dot(lhs[h], leg[h, tt, :, :, lanes].reshape(768, 256),
                        preferred_element_type=F32)
                for h in range(2)
            ]
            for half in range(2):
                a = pa[:, 128 * half:128 * half + 128]
                b = pb[:, 128 * half:128 * half + 128]
                first = jnp.where(low_lanes, a, pltpu.roll(b, 64, 1))
                second = jnp.where(low_lanes, pltpu.roll(a, 64, 1), b)
                for bz, value in ((2 * half, first), (2 * half + 1, second)):
                    q[qs, bx * (1 - par) + bz * par, bz * (1 - par) + bx * par] = value
            if s == 0 and bx is c3:
                send_minus()
            if s == 0 and bx is c1:
                send_plus()
        if s != 0:
            send_minus()
            send_plus()

    def relay1(s):
        par, qs = s % 2, s % 4
        i = x * (1 - par) + z * par
        c1, c3 = (i + 1) % 4, (i + 3) % 4
        send = copies(s, 1, ss1, sr1, par)
        ring(s, 0, ms1, mr1).wait_recv()
        ss1[s, 0] = (q[qs, c3, :, A, :] + mr1[s, 0, 0].astype(F32)).astype(BF)
        send[0].start()
        ss1[s, 1] = (q[qs, c1, :, B, :] + mr1[s, 1, 0].astype(F32)).astype(BF)
        send[1].start()

    def owner1(s):
        par, qs = s % 2, s % 4
        i = x * (1 - par) + z * par
        ring(s, 1, ss1, sr1).wait_recv()
        q2[s, :, A, :] = q[qs, i, :, A, :] + mr1[s, 1, 1].astype(F32) + sr1[s, 0].astype(F32)
        q2[s, :, B, :] = q[qs, i, :, B, :] + mr1[s, 0, 1].astype(F32) + sr1[s, 1].astype(F32)
        j = z * (1 - par) + x * par
        d1, d2, d3 = (j + 1) % 4, (j + 2) % 4, (j + 3) % 4
        if s in DIRECT:
            ss2[s] = q2[s, d2].reshape(2, 128, 128).astype(BF)
            remote(ss2.at[s], sr2.at[s], ring_s.at[s, 3], ring_r.at[s, 3], neighbour(1 - par, 2)).start()
            ms2[s, 0] = q2[s, d3].reshape(2, 128, 128).astype(BF)
            ms2[s, 1] = q2[s, d1].reshape(2, 128, 128).astype(BF)
            for copy in copies(s, 2, ms2, mr2, 1 - par):
                copy.start()
            return
        ms2[s, 0, 0] = q2[s, d2, A, :].astype(BF)
        ms2[s, 0, 1] = q2[s, d3, B, :].astype(BF)
        ms2[s, 1, 0] = q2[s, d2, B, :].astype(BF)
        ms2[s, 1, 1] = q2[s, d1, A, :].astype(BF)
        for copy in copies(s, 2, ms2, mr2, 1 - par):
            copy.start()

    def relay2(s):
        par = s % 2
        j = z * (1 - par) + x * par
        d1, d3 = (j + 1) % 4, (j + 3) % 4
        send = copies(s, 3, ss2, sr2, 1 - par)
        ring(s, 2, ms2, mr2).wait_recv()
        ss2[s, 0] = (q2[s, d3, A, :] + mr2[s, 0, 0].astype(F32)).astype(BF)
        send[0].start()
        ss2[s, 1] = (q2[s, d1, B, :] + mr2[s, 1, 0].astype(F32)).astype(BF)
        send[1].start()

    def owner2(s):
        par = s % 2
        j = z * (1 - par) + x * par
        if s in DIRECT:
            ring(s, 2, ms2, mr2).wait_recv()
            ring(s, 3, ss2, sr2).wait_recv()
            total = mr2[s, 0].astype(F32) + mr2[s, 1].astype(F32) + sr2[s].astype(F32)
            final[s] = q2[s, j] + total.reshape(256, 128)
            return
        ring(s, 3, ss2, sr2).wait_recv()
        final[s, A, :] = q2[s, j, A, :] + mr2[s, 1, 1].astype(F32) + sr2[s, 0].astype(F32)
        final[s, B, :] = q2[s, j, B, :] + mr2[s, 0, 1].astype(F32) + sr2[s, 1].astype(F32)

    def output_group(g):
        top_row = lax.broadcasted_iota(jnp.int32, (8, 128), 0) == 0

        def column(fc, carry):
            pieces = []
            for tt in range(4):
                v0 = final[4 * g + tt, pl.ds(pl.multiple_of(8 * fc, 8), 8), :]
                v1 = final[4 * g + tt, pl.ds(pl.multiple_of(128 + 8 * fc, 8), 8), :]
                if tt % 2:
                    v0, v1 = jnp.where(top_row, v0, v1), jnp.where(top_row, v1, v0)
                pieces += [v0, v1]
            turned = jnp.concatenate(pieces, axis=0).T
            out_row = (fc // 2 * 2 + g) * 2 + fc % 2
            out_ref[pl.ds(out_row, 64, stride=32), :] = jnp.concatenate([turned[0:64], turned[64:128]], axis=1)
            return carry

        lax.fori_loop(0, 16, column, 0, unroll=16)

    def near_group(g):
        for d, other in pairs:
            near(g, d, other).start()

    def far_group(g):
        for d, other in pairs:
            far(g, d, other).start()

    def ring_drain(s, kinds):
        for kind in kinds:
            src, dst = ((ms1, mr1), (ss1, sr1), (ms2, mr2), (ss2, sr2))[kind]
            ring(s, kind, src, dst).wait_send()

    def drain_early():
        for g in range(2):
            all_far(g).wait_send()
            all_near(g).wait_send()
            all_forward(g).wait_send()
            side(g).wait_send()
            for piece in range(PIECES):
                all_order(g, piece).wait_send()
                all_blk(g, piece).wait_send()
        for s in range(4):
            ring_drain(s, (0, 1, 2, 3))
        for s in range(4, 8):
            ring_drain(s, (0,))

    def drain_late():
        for s in range(4, 8):
            ring_drain(s, (1, 2, 3))

    run = dict(F=far_group, N=near_group, P=pass_on, A=transform_group, B=place_group, C=receive_group, M=source_maps,
               m=compute, r=relay1, o=owner1, R=relay2, O=owner2, T=output_group, D=drain_early, E=drain_late)
    for name in SCHEDULE:
        run[name[0]](*map(int, name[1:]))


def analysis(field, mask, plan, legendre):
    high, low = dft_tables()
    vmem, anywhere = pl.BlockSpec(memory_space=pltpu.VMEM), pl.BlockSpec(memory_space=pl.ANY)
    dma = pltpu.SemaphoreType.DMA
    half = (NBLOCK, 2, 4, 128, 128)
    return pl.pallas_call(
        kernel,
        out_shape=pltpu.VMEM((2048, 128), F32),
        in_specs=[anywhere, anywhere, vmem, anywhere, anywhere, anywhere, anywhere],
        out_specs=vmem,
        scratch_shapes=[
            pltpu.VMEM((16, 64, 512), F32),
            pltpu.VMEM((64, 512), jnp.int32),
            pltpu.VMEM((16, 128, 768), BF), pltpu.VMEM((128, 128), BF),
            pltpu.VMEM((2, 8, 64, 512), F32),
            pltpu.VMEM((2, 2, 2, 32, 512), F32),
            pltpu.VMEM((16, 64, 768), BF),
            pltpu.VMEM((128, 1024), BF),
            pltpu.VMEM((2, 8, 8, 16, 128), BF), pltpu.VMEM((2, 8, 8, 16, 128), BF),
            pltpu.VMEM((128, 128), BF), pltpu.VMEM((2, 2, 256, 768), BF),
            pltpu.VMEM((2, 16, 4, 16, 128), BF), pltpu.VMEM((2, 16, 4, 16, 128), BF),
            pltpu.VMEM((2, 4, 48, 16, 1024), BF),
            pltpu.VMEM((4, 4, 4, 256, 128), F32),
            pltpu.VMEM((NBLOCK, 4, 256, 128), F32),
            pltpu.VMEM((NBLOCK, 2, 2, 4, 128, 128), BF), pltpu.VMEM((NBLOCK, 2, 2, 4, 128, 128), BF),
            pltpu.VMEM(half, BF), pltpu.VMEM(half, BF),
            pltpu.VMEM((NBLOCK, 2, 2, 128, 128), BF), pltpu.VMEM((NBLOCK, 2, 2, 128, 128), BF),
            pltpu.VMEM((NBLOCK, 2, 128, 128), BF), pltpu.VMEM((NBLOCK, 2, 128, 128), BF),
            pltpu.VMEM((NBLOCK, 256, 128), F32),
            dma((2,)), dma((4,)), dma((4,)),
            dma((2,)), dma((2, 2, 2)), dma((2,)), dma((2,)), dma((2,)), dma((2,)), dma((2,)), dma((2,)),
            dma((2, PIECES)), dma((2, PIECES)), dma((2, PIECES)), dma((2, PIECES)),
            dma((NBLOCK, 4)), dma((NBLOCK, 4)),
        ],
        compiler_params=pltpu.CompilerParams(collective_id=0, has_side_effects=True, vmem_limit_bytes=62 * 2**20),
    )(field, mask, plan.reshape(8, 128), jnp.asarray(high), jnp.asarray(low), jnp.asarray(order_permutation()), legendre)


def body(field, ocean_mask, plan, legendre):
    return analysis(field, ocean_mask, plan, legendre).reshape(64, 16, 2, 128)


def solution(mesh):
    placed = (P(None, "blk", "order"), P("blk", "order"), P(), P("blk", "order", None))
    return jax.shard_map(
        body, mesh=mesh, in_specs=placed, out_specs=P("blk", None, None, "order"), check_vma=False
    )
```
